32 devices in a mesh: ep: 32 (over z, y, x, core).
Axes of the slice: x: 2, y: 2, z: 4, core: 2. Of those that a mesh axis runs over, the one named last changes fastest.
Arguments:
- x_tokens: bfloat16 [262144, 384], P('ep')
- w_router: float32 [384, 32], replicated
- expert_idx: int32 [262144], P('ep')
- w_in: bfloat16 [32, 384, 1536], P('ep')
- w_out: bfloat16 [32, 1536, 384], P('ep')
- grad_y: bfloat16 [262144, 384], P('ep')
Outputs:
- output 1: bfloat16 [262144, 384], P('ep')
- output 2: float32 [32, 384, 1536], P('ep')
- output 3: float32 [32, 1536, 384], P('ep')
- output 4: float32 [384, 32], replicated
- output 5: float32 [], replicated
- output 6: float32 [], replicated
All inputs are finite; a program needn't handle non-finite values.
Results may differ from the reference program's by a relative error of at most 0.0125986.
Values are sent between devices in bfloat16 or wider.
A program may use at most 1 GiB of HBM per device.

```python
import jax
import jax.numpy as jnp
from jax import lax

D = 384
FF = 1536
EXPERTS = 32
TOKENS = 8192
GROUPS = 32

CAPACITY = (5 * TOKENS + 4 * EXPERTS - 1) // (4 * EXPERTS)
TOTAL_TOK = GROUPS * TOKENS
N_SLOTS = EXPERTS * CAPACITY
AUX_WEIGHT = 0.01
Z_WEIGHT = 0.001
LOGIT_SCALE = 1.5


def draw_routes(route_key):
    key_perm, key_hot, key_tok = jax.random.split(route_key, 3)
    expert_perm = jax.random.permutation(key_perm, EXPERTS)
    hot_expert = jax.random.randint(key_hot, (GROUPS,), 0, EXPERTS)
    n_hot = TOKENS // 4
    n_rest = TOKENS - n_hot - EXPERTS

    def one_group(group_id):
        key_a, key_b, key_c = jax.random.split(jax.random.fold_in(key_tok, group_id), 3)
        first_pick = jax.random.randint(key_a, (n_rest,), 0, EXPERTS)
        second_pick = jax.random.randint(key_b, (n_rest,), 0, EXPERTS)
        skewed = expert_perm[jnp.minimum(first_pick, second_pick)].astype(jnp.int32)
        hot_rows = jnp.full((n_hot,), hot_expert[group_id], jnp.int32)
        listed = jnp.concatenate([hot_rows, jnp.arange(EXPERTS, dtype=jnp.int32), skewed])
        return listed[jax.random.permutation(key_c, TOKENS)]

    return jax.vmap(one_group)(jnp.arange(GROUPS)).reshape(TOTAL_TOK).astype(jnp.int32)


def setup_inputs(seed: int = 0) -> dict:
    base_key = jax.random.key(seed)
    key_x, key_router, key_in, key_out, key_gy, key_route = jax.random.split(base_key, 6)
    x_tokens = jax.random.normal(key_x, (TOTAL_TOK, D), jnp.float32).astype(jnp.bfloat16)
    w_router = jax.random.normal(key_router, (D, EXPERTS), jnp.float32) * (LOGIT_SCALE * D ** -0.5)
    w_in = (jax.random.normal(key_in, (EXPERTS, D, FF), jnp.float32) * D ** -0.5).astype(jnp.bfloat16)
    w_out = (jax.random.normal(key_out, (EXPERTS, FF, D), jnp.float32) * FF ** -0.5).astype(jnp.bfloat16)
    grad_y = jax.random.normal(key_gy, (TOTAL_TOK, D), jnp.float32).astype(jnp.bfloat16)
    expert_idx = draw_routes(key_route)
    return {'x_tokens': x_tokens, 'w_router': w_router, 'expert_idx': expert_idx, 'w_in': w_in, 'w_out': w_out, 'grad_y': grad_y}


def router_group(x_group, w_router, idx_group):
    logits = jnp.dot(x_group.astype(jnp.float32), w_router)
    router_prob = jax.nn.softmax(logits, axis=-1)
    log_norm = jax.nn.logsumexp(logits, axis=-1)
    onehot = (idx_group[:, None] == jnp.arange(EXPERTS)[None, :]).astype(jnp.int32)
    position = jnp.sum(jnp.cumsum(onehot, axis=0) * onehot, axis=1) - 1
    tok_slot = jnp.where(position < CAPACITY, idx_group * CAPACITY + position, N_SLOTS)
    onehot_f = onehot.astype(jnp.float32)
    gate_val = jnp.sum(router_prob * onehot_f, axis=-1)
    return router_prob, log_norm, onehot_f, gate_val, tok_slot


def reference(x_tokens, w_router, expert_idx, w_in, w_out, grad_y):
    x_groups = x_tokens.reshape(GROUPS, TOKENS, D)
    idx_groups = expert_idx.reshape(GROUPS, TOKENS)
    gy_groups = grad_y.reshape(GROUPS, TOKENS, D)

    def first_pass(operands):
        x_group, idx_group, gy_group = operands
        router_prob, log_norm, onehot_f, gate_val, tok_slot = router_group(x_group, w_router, idx_group)
        scaled = (gate_val[:, None] * gy_group.astype(jnp.float32)).astype(jnp.bfloat16)
        empty_buf = jnp.zeros((N_SLOTS + 1, D), jnp.bfloat16)
        sent_rows = empty_buf.at[tok_slot].set(x_group)[:N_SLOTS]
        sent_grad = empty_buf.at[tok_slot].set(scaled)[:N_SLOTS]
        route_stats = jnp.concatenate([jnp.sum(onehot_f, axis=0), jnp.sum(router_prob, axis=0), jnp.sum(log_norm * log_norm)[None]])
        return sent_rows, sent_grad, route_stats

    sent_rows, sent_grad, route_stats = lax.map(first_pass, (x_groups, idx_groups, gy_groups))
    rows_all = sent_rows.reshape(GROUPS, EXPERTS, CAPACITY, D).transpose(1, 0, 2, 3).reshape(EXPERTS, GROUPS * CAPACITY, D)
    grads_all = sent_grad.reshape(GROUPS, EXPERTS, CAPACITY, D).transpose(1, 0, 2, 3).reshape(EXPERTS, GROUPS * CAPACITY, D)

    def expert_pass(operands):
        recv_rows, recv_grad, w_first, w_second = operands
        pre_act = jnp.dot(recv_rows, w_first, preferred_element_type=jnp.float32)
        hidden = jnp.maximum(pre_act, 0.0).astype(jnp.bfloat16)
        expert_out = jnp.dot(hidden, w_second, preferred_element_type=jnp.float32).astype(jnp.bfloat16)
        d_hidden = jnp.dot(recv_grad, w_second.T, preferred_element_type=jnp.float32)
        d_pre = jnp.where(hidden > 0, d_hidden, 0.0).astype(jnp.bfloat16)
        grad_out_e = jnp.dot(hidden.T, recv_grad, preferred_element_type=jnp.float32)
        grad_in_e = jnp.dot(recv_rows.T, d_pre, preferred_element_type=jnp.float32)
        d_rows = jnp.dot(d_pre, w_first.T, preferred_element_type=jnp.float32).astype(jnp.bfloat16)
        return expert_out, d_rows, grad_in_e, grad_out_e

    expert_out, d_rows, grad_w_in, grad_w_out = lax.map(expert_pass, (rows_all, grads_all, w_in, w_out))
    out_groups = expert_out.reshape(EXPERTS, GROUPS, CAPACITY, D).transpose(1, 0, 2, 3).reshape(GROUPS, N_SLOTS, D)
    back_groups = d_rows.reshape(EXPERTS, GROUPS, CAPACITY, D).transpose(1, 0, 2, 3).reshape(GROUPS, N_SLOTS, D)

    totals = jnp.sum(route_stats, axis=0)
    load_frac = totals[:EXPERTS] / TOTAL_TOK
    mean_prob = totals[EXPERTS:2 * EXPERTS] / TOTAL_TOK
    aux_loss = AUX_WEIGHT * EXPERTS * jnp.sum(load_frac * mean_prob)
    z_loss = Z_WEIGHT * totals[2 * EXPERTS] / TOTAL_TOK
    aux_vec = AUX_WEIGHT * EXPERTS * load_frac / TOTAL_TOK
    z_coef = 2.0 * Z_WEIGHT / TOTAL_TOK
    pad_row = jnp.zeros((1, D), jnp.bfloat16)

    def second_pass(operands):
        x_group, idx_group, gy_group, out_group, back_group = operands
        router_prob, log_norm, onehot_f, gate_val, tok_slot = router_group(x_group, w_router, idx_group)
        out_tok = jnp.concatenate([out_group, pad_row])[tok_slot]
        back_tok = jnp.concatenate([back_group, pad_row])[tok_slot]
        d_gate = jnp.sum(out_tok.astype(jnp.float32) * gy_group.astype(jnp.float32), axis=-1)
        spread = jnp.sum(router_prob * aux_vec[None, :], axis=-1, keepdims=True)
        d_logits = ((gate_val * d_gate)[:, None] * (onehot_f - router_prob)
                    + router_prob * (aux_vec[None, :] - spread)
                    + (z_coef * log_norm)[:, None] * router_prob)
        grad_x = (back_tok.astype(jnp.float32) + jnp.dot(d_logits, w_router.T)).astype(jnp.bfloat16)
        part_router = jnp.dot(x_group.astype(jnp.float32).T, d_logits)
        return grad_x, part_router

    grad_x, parts_router = lax.map(second_pass, (x_groups, idx_groups, gy_groups, out_groups, back_groups))
    return grad_x.reshape(TOTAL_TOK, D), grad_w_in, grad_w_out, jnp.sum(parts_router, axis=0), aux_loss, z_loss
```

```python
import jax
import jax.numpy as jnp
from jax import lax
from jax.sharding import PartitionSpec as P

AUX_WEIGHT = 0.01
Z_WEIGHT = 0.001
BF = jnp.bfloat16
F32 = jnp.float32


def gather_rows(source, row_index):
    return jnp.take(source, row_index, axis=0, mode='fill', fill_value=0)


def solution(mesh):
    n_dev = mesh.shape['ep']
    hd = n_dev // 2
    groups = [list(range(hd)), list(range(hd, n_dev))]
    mirror = [(i, (i + hd) % n_dev) for i in range(n_dev)]

    def a2a(v):
        return lax.all_to_all(v, 'ep', 0, 0, tiled=True, axis_index_groups=groups)

    def expert_layer(x_tokens, w_router, expert_idx, w_in, w_out, grad_y):
        tokens, d_model = x_tokens.shape
        ne = n_dev
        capacity = (5 * tokens + 4 * ne - 1) // (4 * ne)
        total_tok = tokens * n_dev
        n_slots = ne * capacity
        me = lax.axis_index('ep')
        half = me // hd
        w_in_o, w_out_o = w_in[0], w_out[0]
        w_in_m = lax.ppermute(w_in_o, 'ep', mirror)
        w_out_m = lax.ppermute(w_out_o, 'ep', mirror)

        onehot = (expert_idx[:, None] == jnp.arange(ne, dtype=jnp.int32)[None, :]).astype(jnp.int32)
        position = jnp.sum(jnp.cumsum(onehot, axis=0) * onehot, axis=1) - 1
        rel = (expert_idx + hd * half) % ne
        kept = position < capacity
        tok_slot = jnp.where(kept, rel * capacity + position, n_slots)
        slot_tok = jnp.full((n_slots,), tokens, jnp.int32).at[tok_slot].set(jnp.arange(tokens, dtype=jnp.int32), mode='drop')
        counts = jnp.sum(onehot, axis=0).astype(F32)
        load_frac = lax.psum(counts, 'ep') / total_tok
        aux_vec = AUX_WEIGHT * ne * load_frac / total_tok
        z_coef = 2.0 * Z_WEIGHT / total_tok

        def router(rows):
            logits = jnp.dot(rows, w_router, preferred_element_type=F32)
            return jax.nn.softmax(logits, axis=-1), jax.nn.logsumexp(logits, axis=-1)

        def base_grad(p, lz):
            spread = jnp.sum(p * aux_vec, axis=-1, keepdims=True)
            return p * (aux_vec - spread) + (z_coef * lz)[:, None] * p

        def expert(xr, dyr, wi, wo, e_id):
            p, lz = router(xr)
            hot = (jnp.arange(ne) == e_id).astype(F32)
            gate = jnp.sum(p * hot, axis=-1)
            dyf = dyr.astype(F32)
            g = (gate[:, None] * dyf).astype(BF)
            h = jnp.maximum(jnp.dot(xr, wi, preferred_element_type=F32), 0.0).astype(BF)
            o = jnp.dot(h, wo, preferred_element_type=F32).astype(BF)
            dgate = jnp.sum(o.astype(F32) * dyf, axis=-1)
            dh = jnp.einsum('td,fd->tf', g, wo, preferred_element_type=F32)
            da = jnp.where(h > 0, dh, 0.0).astype(BF)
            gwo = jnp.einsum('tf,td->fd', h, g, preferred_element_type=F32)
            gwi = jnp.einsum('td,tf->df', xr, da, preferred_element_type=F32)
            dr = jnp.einsum('tf,df->td', da, wi, preferred_element_type=F32).astype(BF)
            dl = (gate * dgate)[:, None] * (hot - p) + base_grad(p, lz)
            gx = (dr.astype(F32) + jnp.einsum('te,de->td', dl, w_router)).astype(BF)
            gwr = jnp.einsum('td,te->de', xr, dl, preferred_element_type=F32)
            return gx, gwi, gwo, gwr

        hs = hd * capacity
        xm = a2a(gather_rows(x_tokens, slot_tok[hs:]))
        dym = a2a(gather_rows(grad_y, slot_tok[hs:]))
        xo = a2a(gather_rows(x_tokens, slot_tok[:hs]))
        dyo = a2a(gather_rows(grad_y, slot_tok[:hs]))
        gx_m, gwi_m, gwo_m, gwr_m = expert(xm, dym, w_in_m, w_out_m, (me + hd) % n_dev)
        gwi_r = lax.ppermute(gwi_m, 'ep', mirror)
        gwo_r = lax.ppermute(gwo_m, 'ep', mirror)
        back_m = a2a(gx_m)
        gx_o, gwi_o, gwo_o, gwr_o = expert(xo, dyo, w_in_o, w_out_o, me)
        back_o = a2a(gx_o)

        p, lz = router(x_tokens)
        dl = base_grad(p, lz)
        gx_drop = jnp.einsum('te,de->td', dl, w_router).astype(BF)
        gwr_d = jnp.einsum('td,te->de', x_tokens, jnp.where(kept[:, None], 0.0, dl), preferred_element_type=F32)
        back = jnp.concatenate([back_o, back_m], axis=0)
        rows = jnp.take(back, jnp.minimum(tok_slot, n_slots - 1), axis=0, mode='clip')
        grad_x = jnp.where(kept[:, None], rows, gx_drop)
        fin = jnp.concatenate([(gwr_d + gwr_m + gwr_o).reshape(-1), jnp.sum(p, axis=0), jnp.sum(lz * lz)[None]])
        fin = lax.psum(fin, 'ep')
        nr = d_model * ne
        grad_w_router = fin[:nr].reshape(d_model, ne)
        aux_loss = AUX_WEIGHT * ne * jnp.sum(load_frac * fin[nr:nr + ne] / total_tok)
        z_loss = Z_WEIGHT * fin[nr + ne] / total_tok
        return grad_x, (gwi_o + gwi_r)[None], (gwo_o + gwo_r)[None], grad_w_router, aux_loss, z_loss

    return jax.shard_map(expert_layer, mesh=mesh,
                         in_specs=(P('ep', None), P(None, None), P('ep'), P('ep', None, None), P('ep', None, None), P('ep', None)),
                         out_specs=(P('ep', None), P('ep', None, None), P('ep', None, None), P(None, None), P(), P()),
                         check_vma=False)
```

```python
import functools
import jax
import jax.numpy as jnp
from jax import lax
from jax.experimental import pallas as pl
from jax.experimental.pallas import tpu as pltpu
from jax.sharding import PartitionSpec as P

AUX_WEIGHT = 0.01
Z_WEIGHT = 0.001
BF = jnp.bfloat16
F32 = jnp.float32
LANES = 128
MESH_ID = pl.DeviceIdType.MESH
VMEM_LIMIT = 60 * 1024 * 1024


def gather_rows(source, row_index):
    return jnp.take(source, row_index, axis=0, mode='fill', fill_value=0)


def xor3(a, b):
    out = 0
    for k in (1, 2, 4):
        out = out + k * lax.rem(a // k + b // k, 2)
    return out


def dot(a, b, ca=1, cb=0):
    return lax.dot_general(a, b, (((ca,), (cb,)), ((), ())), preferred_element_type=F32)


def expert_kernel(cfg, *refs):
    n_dev, hd, cap, d, ff, ft, total_tok, first = cfg
    if first:
        (cnt_ref, sx, sdy, wi, wo, wr, wrt,
         gx_out, gwi, gwo, gwr, tot_ref,
         xr, dyr, gwot, dlw, oacc, dracc, gb, xt, gt, stage,
         cbuf, csend, crecv, loc_sem, send_sem, recv_sem, out_sem) = refs
    else:
        (tot_in, gxm, sx, sdy, wi, wo, wr, wrt,
         back_m, back_o, gwi, gwo, gwr,
         xr, dyr, gwot, dlw, oacc, dracc, gb, xt, gt, stage,
         loc_sem, send_sem, recv_sem, out_sem, bm_send, bm_recv, bo_send, bo_recv) = refs
    me = lax.axis_index('ep')
    half = me // hd
    rank = lax.rem(me, hd)
    chip = rank // 2
    core = lax.rem(rank, 2)
    n_grp = hd // 2
    rows = 2 * cap

    def peer_of(j, c):
        return xor3(chip, j) * 2 + lax.rem(core + c, 2)

    def token_copy(a, src, dst, peer):
        return pltpu.make_async_remote_copy(
            src_ref=src.at[peer], dst_ref=dst.at[rank], send_sem=send_sem.at[a, peer],
            recv_sem=recv_sem.at[a, rank], device_id=(half * hd + peer,), device_id_type=MESH_ID)

    def token_wait(a, src, dst, peer):
        return pltpu.make_async_remote_copy(
            src_ref=src.at[peer], dst_ref=dst.at[peer], send_sem=send_sem.at[a, peer],
            recv_sem=recv_sem.at[a, peer], device_id=(half * hd + peer,), device_id_type=MESH_ID)

    def back_copy(src, dst, ssem, rsem, peer):
        return pltpu.make_async_remote_copy(
            src_ref=src.at[peer], dst_ref=dst.at[rank], send_sem=ssem.at[peer],
            recv_sem=rsem.at[rank], device_id=(half * hd + peer,), device_id_type=MESH_ID)

    def back_wait(src, dst, ssem, rsem, peer):
        return pltpu.make_async_remote_copy(
            src_ref=src.at[peer], dst_ref=dst.at[peer], send_sem=ssem.at[peer],
            recv_sem=rsem.at[peer], device_id=(half * hd + peer,), device_id_type=MESH_ID)

    if first:
        def count_send(k):
            peer = lax.rem(me + k, n_dev)
            return pltpu.make_async_remote_copy(
                src_ref=cnt_ref, dst_ref=cbuf.at[me], send_sem=csend.at[peer],
                recv_sem=crecv.at[me], device_id=(peer,), device_id_type=MESH_ID)

        def count_wait(k):
            peer = lax.rem(me + k, n_dev)
            return pltpu.make_async_remote_copy(
                src_ref=cnt_ref, dst_ref=cbuf.at[peer], send_sem=csend.at[peer],
                recv_sem=crecv.at[peer], device_id=(peer,), device_id_type=MESH_ID)

        def start_count(k, _):
            count_send(k).start()
            return 0
        lax.fori_loop(1, n_dev, start_count, 0)
        cbuf[me] = cnt_ref[...]

    own_x = pltpu.make_async_copy(sx.at[rank], xr.at[rank], loc_sem.at[0])
    own_dy = pltpu.make_async_copy(sdy.at[rank], dyr.at[rank], loc_sem.at[1])
    own_x.start()
    own_dy.start()

    def start_peer(peer):
        token_copy(0, sx, xr, peer).start()
        token_copy(1, sdy, dyr, peer).start()
        if not first:
            back_copy(gxm, back_m, bm_send, bm_recv, peer).start()

    start_peer(peer_of(0, 1))

    def start_group(j, _):
        start_peer(peer_of(j, 0))
        start_peer(peer_of(j, 1))
        return 0
    lax.fori_loop(1, n_grp, start_group, 0)
    if not first:
        own_bm = pltpu.make_async_copy(gxm.at[rank], back_m.at[rank], loc_sem.at[2])
        own_bm.start()

    gwi[...] = jnp.zeros_like(gwi)
    gwot[...] = jnp.zeros_like(gwot)
    gwr[...] = jnp.zeros_like(gwr)

    if first:
        def wait_count(k, _):
            count_wait(k).wait_recv()
            return 0
        lax.fori_loop(1, n_dev, wait_count, 0)
        tot_ref[...] = jnp.sum(cbuf[...], axis=0)
        tot = tot_ref[0:1, :]
        e_id = lax.rem(me + hd, n_dev)
    else:
        tot = tot_in[0:1, :]
        e_id = me
    v = tot * (AUX_WEIGHT * n_dev / (float(total_tok) * total_tok))
    zc = 2.0 * Z_WEIGHT / total_tok

    def group(j, _):
        @pl.when(j == 0)
        def _():
            own_x.wait()
            own_dy.wait()

        @pl.when(j > 0)
        def _():
            token_wait(0, sx, xr, peer_of(j, 0)).wait_recv()
            token_wait(1, sdy, dyr, peer_of(j, 0)).wait_recv()
        token_wait(0, sx, xr, peer_of(j, 1)).wait_recv()
        token_wait(1, sdy, dyr, peer_of(j, 1)).wait_recv()
        pair = xor3(chip, j)
        x = xr[pl.ds(2 * pair, 2)].reshape(rows, d)
        dyf = dyr[pl.ds(2 * pair, 2)].reshape(rows, d).astype(F32)
        lane = lax.broadcasted_iota(jnp.int32, (rows, LANES), 1)
        lg = dot(x, wr[...])
        lg = lg[:, :LANES] + lg[:, LANES:]
        lg = jnp.where(lane < n_dev, lg, -1e30)
        mx = jnp.max(lg, axis=1, keepdims=True)
        ex = jnp.exp(lg - mx)
        sm = jnp.sum(ex, axis=1, keepdims=True)
        p = ex / sm
        lz = mx + jnp.log(sm)
        hot = (lane == e_id).astype(F32)
        gate = jnp.sum(p * hot, axis=1, keepdims=True)
        g = (gate * dyf).astype(BF)
        gb[...] = g
        xt[...] = x.T
        gt[...] = g.T
        oacc[...] = jnp.zeros_like(oacc)
        dracc[...] = jnp.zeros_like(dracc)

        def ff_tile(f, _):
            fo = pl.multiple_of(f * ft, ft)
            wit = wi[:, pl.ds(fo, ft)]
            wot = wo[pl.ds(fo, ft), :]
            xx = xr[pl.ds(2 * pair, 2)].reshape(rows, d)
            h = jnp.maximum(dot(xx, wit), 0.0).astype(BF)
            oacc[...] += dot(h, wot)
            dh = dot(gb[...], wot, 1, 1)
            da = jnp.where(h > 0, dh, 0.0).astype(BF)
            dracc[...] += dot(da, wit, 1, 1)
            gwot[:, pl.ds(fo, ft)] += dot(gt[...], h)
            gwi[:, pl.ds(fo, ft)] += dot(xt[...], da)
            return 0
        lax.fori_loop(0, ff // ft, ff_tile, 0)

        o = oacc[...].astype(BF).astype(F32)
        dgate = jnp.sum(o * dyf, axis=1, keepdims=True)
        spread = jnp.sum(p * v, axis=1, keepdims=True)
        dl = (gate * dgate) * (hot - p) + p * (v - spread) + (zc * lz) * p
        dl_hi = dl.astype(BF)
        dl_lo = (dl - dl_hi.astype(F32)).astype(BF)
        dl2 = jnp.concatenate([dl_hi, dl_lo], axis=1)
        dlw[...] = dot(jnp.concatenate([dl2, dl_hi], axis=1), wrt[...])
        gw = dot(xt[...], dl2)
        gwr[...] += gw[:, :LANES] + gw[:, LANES:]
        gx = (dracc[...].astype(BF).astype(F32) + dlw[...]).astype(BF)
        stage[pl.ds(2 * pair, 2)] = gx.reshape(2, cap, d)
        for c in (0, 1):
            peer = peer_of(j, c)
            if first:
                pltpu.make_async_copy(stage.at[peer], gx_out.at[peer], out_sem.at[peer]).start()
            elif c == 1:
                back_copy(stage, back_o, bo_send, bo_recv, peer).start()
            else:
                @pl.when(j == 0)
                def _():
                    pltpu.make_async_copy(stage.at[rank], back_o.at[rank], out_sem.at[0]).start()

                @pl.when(j > 0)
                def _():
                    back_copy(stage, back_o, bo_send, bo_recv, peer).start()
        return 0
    lax.fori_loop(0, n_grp, group, 0)

    def finish(f, _):
        fo = pl.multiple_of(f * ft, ft)
        gwo[pl.ds(fo, ft), :] = gwot[:, pl.ds(fo, ft)].T
        return 0
    lax.fori_loop(0, ff // ft, finish, 0)

    def drain_peer(peer):
        token_wait(0, sx, xr, peer).wait_send()
        token_wait(1, sdy, dyr, peer).wait_send()
        if not first:
            back_wait(gxm, back_m, bm_send, bm_recv, peer).wait_send()
            back_wait(gxm, back_m, bm_send, bm_recv, peer).wait_recv()
            back_wait(stage, back_o, bo_send, bo_recv, peer).wait_send()
            back_wait(stage, back_o, bo_send, bo_recv, peer).wait_recv()

    drain_peer(peer_of(0, 1))

    def drain(j, _):
        drain_peer(peer_of(j, 0))
        drain_peer(peer_of(j, 1))
        return 0
    lax.fori_loop(1, n_grp, drain, 0)
    if first:
        def out_wait(s, _):
            pltpu.make_async_copy(stage.at[s], gx_out.at[s], out_sem.at[s]).wait()
            return 0
        lax.fori_loop(0, hd, out_wait, 0)

        def count_drain(k, _):
            count_wait(k).wait_send()
            return 0
        lax.fori_loop(1, n_dev, count_drain, 0)
    else:
        own_bm.wait()
        pltpu.make_async_copy(stage.at[rank], back_o.at[rank], out_sem.at[0]).wait()


def expert_call(cfg, *args):
    n_dev, hd, cap, d, ff, ft, total_tok, first = cfg
    vm = pl.BlockSpec(memory_space=pltpu.VMEM)
    hbm = pl.BlockSpec(memory_space=pltpu.HBM)
    sd = jax.ShapeDtypeStruct
    rows = 2 * cap
    tok = sd((hd, cap, d), BF)
    grads = [sd((d, ff), F32), sd((ff, d), F32), sd((d, LANES), F32)]
    dma = pltpu.SemaphoreType.DMA
    scratch = [pltpu.VMEM((hd, cap, d), BF), pltpu.VMEM((hd, cap, d), BF), pltpu.VMEM((d, ff), F32),
               pltpu.VMEM((rows, d), F32), pltpu.VMEM((rows, d), F32), pltpu.VMEM((rows, d), F32),
               pltpu.VMEM((rows, d), BF), pltpu.VMEM((d, rows), BF), pltpu.VMEM((d, rows), BF),
               pltpu.VMEM((hd, cap, d), BF)]
    common = [dma((3,)), dma((2, hd)), dma((2, hd)), dma((hd,))]
    if first:
        in_specs = [vm, hbm, hbm, vm, vm, vm, vm]
        out_shape = [tok] + grads + [sd((8, LANES), F32)]
        out_specs = [hbm, vm, vm, vm, vm]
        scratch += [pltpu.VMEM((n_dev, 8, LANES), F32), dma((n_dev,)), dma((n_dev,))] + common
    else:
        in_specs = [vm, hbm, hbm, hbm, vm, vm, vm, vm]
        out_shape = [tok, tok] + grads
        out_specs = [hbm, hbm, vm, vm, vm]
        scratch += common + [dma((hd,))] * 4
    return pl.pallas_call(
        functools.partial(expert_kernel, cfg), out_shape=out_shape, in_specs=in_specs, out_specs=out_specs,
        scratch_shapes=scratch, name='expert_a' if first else 'expert_b',
        cost_estimate=pl.CostEstimate(flops=12 * hd * cap * d * ff, bytes_accessed=32 * 2 ** 20, transcendentals=0),
        compiler_params=pltpu.CompilerParams(has_side_effects=True, vmem_limit_bytes=VMEM_LIMIT))(*args)


def split_router(w_router):
    d, ne = w_router.shape
    hi = lax.reduce_precision(w_router, 8, 7)
    lo = lax.reduce_precision(w_router - hi, 8, 7)
    pad = lambda a: jnp.pad(a, ((0, 0), (0, LANES - ne)))
    wr = jnp.concatenate([pad(hi), pad(lo)], axis=1).astype(BF)
    wrt = jnp.concatenate([pad(hi), pad(hi), pad(lo)], axis=1).T.astype(BF)
    return wr, wrt


def solution(mesh):
    n_dev = mesh.shape['ep']
    hd = n_dev // 2
    mirror = [(i, (i + hd) % n_dev) for i in range(n_dev)]

    def expert_layer(x_tokens, w_router, expert_idx, w_in, w_out, grad_y):
        tokens, d_model = x_tokens.shape
        ff = w_in.shape[-1]
        ne = n_dev
        capacity = (5 * tokens + 4 * ne - 1) // (4 * ne)
        total_tok = tokens * n_dev
        n_slots = ne * capacity
        me = lax.axis_index('ep')
        half = me // hd
        w_in_o, w_out_o = w_in[0], w_out[0]
        w_in_m = lax.ppermute(w_in_o, 'ep', mirror)
        w_out_m = lax.ppermute(w_out_o, 'ep', mirror)
        wr, wrt = split_router(w_router)

        onehot = (expert_idx[:, None] == jnp.arange(ne, dtype=jnp.int32)[None, :]).astype(jnp.int32)
        position = jnp.sum(jnp.cumsum(onehot, axis=0) * onehot, axis=1) - 1
        rel = (expert_idx + hd * half) % ne
        kept = position < capacity
        tok_slot = jnp.where(kept, rel * capacity + position, n_slots)
        slot_tok = jnp.full((n_slots,), tokens, jnp.int32).at[tok_slot].set(jnp.arange(tokens, dtype=jnp.int32), mode='drop')
        counts = jnp.sum(onehot, axis=0).astype(F32)
        cnt = jnp.broadcast_to(jnp.pad(counts, (0, LANES - ne))[None], (8, LANES))

        hs = hd * capacity
        shape = (hd, capacity, d_model)
        base = (n_dev, hd, capacity, d_model, ff, 512, total_tok)
        xm = gather_rows(x_tokens, slot_tok[hs:]).reshape(shape)
        dym = gather_rows(grad_y, slot_tok[hs:]).reshape(shape)
        gx_m, gwi_m, gwo_m, gwr_m, tot = expert_call(base + (True,), cnt, xm, dym, w_in_m, w_out_m, wr, wrt)
        gwi_r = lax.ppermute(gwi_m, 'ep', mirror)
        gwo_r = lax.ppermute(gwo_m, 'ep', mirror)
        xo = gather_rows(x_tokens, slot_tok[:hs]).reshape(shape)
        dyo = gather_rows(grad_y, slot_tok[:hs]).reshape(shape)
        back_m, back_o, gwi_o, gwo_o, gwr_o = expert_call(base + (False,), tot, gx_m, xo, dyo, w_in_o, w_out_o, wr, wrt)

        load_frac = tot[0, :ne] / total_tok
        aux_vec = AUX_WEIGHT * ne * load_frac / total_tok
        z_coef = 2.0 * Z_WEIGHT / total_tok
        logits = jnp.dot(x_tokens, w_router, preferred_element_type=F32)
        p = jax.nn.softmax(logits, axis=-1)
        lz = jax.nn.logsumexp(logits, axis=-1)
        dl = p * (aux_vec - jnp.sum(p * aux_vec, axis=-1, keepdims=True)) + (z_coef * lz)[:, None] * p
        gx_drop = jnp.einsum('te,de->td', dl, w_router).astype(BF)
        gwr_d = jnp.einsum('td,te->de', x_tokens, jnp.where(kept[:, None], 0.0, dl), preferred_element_type=F32)
        back = jnp.concatenate([back_o, back_m], axis=0).reshape(n_slots, d_model)
        rows = jnp.take(back, jnp.minimum(tok_slot, n_slots - 1), axis=0, mode='clip')
        grad_x = jnp.where(kept[:, None], rows, gx_drop)
        fin = jnp.concatenate([(gwr_d + (gwr_m + gwr_o)[:, :ne]).reshape(-1), jnp.sum(p, axis=0), jnp.sum(lz * lz)[None]])
        fin = lax.psum(fin, 'ep')
        nr = d_model * ne
        grad_w_router = fin[:nr].reshape(d_model, ne)
        aux_loss = AUX_WEIGHT * ne * jnp.sum(load_frac * fin[nr:nr + ne] / total_tok)
        z_loss = Z_WEIGHT * fin[nr + ne] / total_tok
        return grad_x, (gwi_o + gwi_r)[None], (gwo_o + gwo_r)[None], grad_w_router, aux_loss, z_loss

    return jax.shard_map(expert_layer, mesh=mesh,
                         in_specs=(P('ep', None), P(None, None), P('ep'), P('ep', None, None), P('ep', None, None), P('ep', None)),
                         out_specs=(P('ep', None), P('ep', None, None), P('ep', None, None), P(None, None), P(), P()),
                         check_vma=False)
```

```python
import functools
import jax
import jax.numpy as jnp
from jax import lax
from jax.experimental import pallas as pl
from jax.experimental.pallas import tpu as pltpu
from jax.sharding import PartitionSpec as P

AUX_WEIGHT = 0.01
Z_WEIGHT = 0.001
BF = jnp.bfloat16
F32 = jnp.float32
LANES = 128
MESH_ID = pl.DeviceIdType.MESH
VMEM_LIMIT = 60 * 1024 * 1024
VM = pl.BlockSpec(memory_space=pltpu.VMEM)
SM = pl.BlockSpec(memory_space=pltpu.SMEM)
HBM = pl.BlockSpec(memory_space=pltpu.HBM)


def xor3(a, b):
    out = 0
    for k in (1, 2, 4):
        out = out + k * lax.rem(a // k + b // k, 2)
    return out


def dot(a, b, ca=1, cb=0):
    return lax.dot_general(a, b, (((ca,), (cb,)), ((), ())), preferred_element_type=F32)


def expert_kernel(cfg, *refs):
    n_dev, hd, cap, d, ff, ft, total_tok, first = cfg
    lead, sx, sdy, wi, wo, wr, wrt, gx_out, gwi, gwo, gwr = refs[:11]
    rest = refs[11:]
    if first:
        tot_ref, cbuf, csend, crecv = rest[0], *rest[1:4]
        rest = rest[4:]
    xr, dyr, gwot, dlw, oacc, dracc, gb, xt, gt, stage, loc_sem, send_sem, recv_sem, out_sem = rest
    me = lax.axis_index('ep')
    half = me // hd
    rank = lax.rem(me, hd)
    chip = rank // 2
    core = lax.rem(rank, 2)
    n_grp = hd // 2
    rows = 2 * cap
    off = 0 if first else hd

    def peer_of(j, c):
        return xor3(chip, j) * 2 + lax.rem(core + c, 2)

    def token_copy(a, src, dst, peer, slot):
        return pltpu.make_async_remote_copy(
            src_ref=src.at[off + peer], dst_ref=dst.at[slot], send_sem=send_sem.at[a, peer],
            recv_sem=recv_sem.at[a, slot], device_id=(half * hd + peer,), device_id_type=MESH_ID)

    if first:
        def count_copy(k, sending):
            peer = lax.rem(me + k, n_dev)
            slot = me if sending else peer
            return pltpu.make_async_remote_copy(
                src_ref=lead, dst_ref=cbuf.at[slot], send_sem=csend.at[peer],
                recv_sem=crecv.at[slot], device_id=(peer,), device_id_type=MESH_ID)

        def start_count(k, _):
            count_copy(k, True).start()
            return 0
        lax.fori_loop(1, n_dev, start_count, 0)
        cbuf[me] = lead[...]

    own_x = pltpu.make_async_copy(sx.at[off + rank], xr.at[rank], loc_sem.at[0])
    own_dy = pltpu.make_async_copy(sdy.at[off + rank], dyr.at[rank], loc_sem.at[1])
    own_x.start()
    own_dy.start()

    def start_peer(peer):
        token_copy(0, sx, xr, peer, rank).start()
        token_copy(1, sdy, dyr, peer, rank).start()

    start_peer(peer_of(0, 1))

    def start_group(j, _):
        start_peer(peer_of(j, 0))
        start_peer(peer_of(j, 1))
        return 0
    lax.fori_loop(1, n_grp, start_group, 0)

    gwi[...] = jnp.zeros_like(gwi)
    gwot[...] = jnp.zeros_like(gwot)
    gwr[...] = jnp.zeros_like(gwr)

    if first:
        def wait_count(k, _):
            count_copy(k, False).wait_recv()
            return 0
        lax.fori_loop(1, n_dev, wait_count, 0)
        tot_ref[...] = jnp.sum(cbuf[...], axis=0)
        tot = tot_ref[0:1, :]
        e_id = me
    else:
        tot = lead[0:1, :]
        e_id = lax.rem(me + hd, n_dev)
    v = tot * (AUX_WEIGHT * n_dev / (float(total_tok) * total_tok))
    zc = 2.0 * Z_WEIGHT / total_tok

    def recv_wait(peer):
        token_copy(0, sx, xr, peer, peer).wait_recv()
        token_copy(1, sdy, dyr, peer, peer).wait_recv()

    def group(j, _):
        @pl.when(j == 0)
        def _():
            own_x.wait()
            own_dy.wait()

        @pl.when(j > 0)
        def _():
            recv_wait(peer_of(j, 0))
        recv_wait(peer_of(j, 1))
        pair = xor3(chip, j)
        x = xr[pl.ds(2 * pair, 2)].reshape(rows, d)
        dyf = dyr[pl.ds(2 * pair, 2)].reshape(rows, d).astype(F32)
        lane = lax.broadcasted_iota(jnp.int32, (rows, LANES), 1)
        p, lz = router_rows(x, wr, lane, n_dev)
        hot = (lane == e_id).astype(F32)
        gate = jnp.sum(p * hot, axis=1, keepdims=True)
        g = (gate * dyf).astype(BF)
        gb[...] = g
        xt[...] = x.T
        gt[...] = g.T
        oacc[...] = jnp.zeros_like(oacc)
        dracc[...] = jnp.zeros_like(dracc)

        def ff_tile(f, _):
            fo = pl.multiple_of(f * ft, ft)
            wit = wi[:, pl.ds(fo, ft)]
            wot = wo[pl.ds(fo, ft), :]
            xx = xr[pl.ds(2 * pair, 2)].reshape(rows, d)
            h = jnp.maximum(dot(xx, wit), 0.0).astype(BF)
            oacc[...] += dot(h, wot)
            dh = dot(gb[...], wot, 1, 1)
            da = jnp.where(h > 0, dh, 0.0).astype(BF)
            dracc[...] += dot(da, wit, 1, 1)
            gwot[:, pl.ds(fo, ft)] += dot(gt[...], h)
            gwi[:, pl.ds(fo, ft)] += dot(xt[...], da)
            return 0
        lax.fori_loop(0, ff // ft, ff_tile, 0)

        o = oacc[...].astype(BF).astype(F32)
        dgate = jnp.sum(o * dyf, axis=1, keepdims=True)
        dl = (gate * dgate) * (hot - p) + base_grad(p, lz, v, zc)
        dl2, dl3 = split_rows(dl)
        dlw[...] = dot(dl3, wrt[...])
        gw = dot(xt[...], dl2)
        gwr[...] += gw[:, :LANES] + gw[:, LANES:]
        gx = (dracc[...].astype(BF).astype(F32) + dlw[...]).astype(BF)
        stage[pl.ds(2 * pair, 2)] = gx.reshape(2, cap, d)
        pltpu.make_async_copy(stage.at[pl.ds(2 * pair, 2)], gx_out.at[pl.ds(2 * pair, 2)], out_sem.at[pair]).start()
        return 0
    lax.fori_loop(0, n_grp, group, 0)

    def finish(f, _):
        fo = pl.multiple_of(f * ft, ft)
        gwo[pl.ds(fo, ft), :] = gwot[:, pl.ds(fo, ft)].T
        return 0
    lax.fori_loop(0, ff // ft, finish, 0)

    def send_wait(peer):
        token_copy(0, sx, xr, peer, peer).wait_send()
        token_copy(1, sdy, dyr, peer, peer).wait_send()

    send_wait(peer_of(0, 1))

    def drain(j, _):
        send_wait(peer_of(j, 0))
        send_wait(peer_of(j, 1))
        return 0
    lax.fori_loop(1, n_grp, drain, 0)

    def out_wait(s, _):
        pltpu.make_async_copy(stage.at[pl.ds(2 * s, 2)], gx_out.at[pl.ds(2 * s, 2)], out_sem.at[s]).wait()
        return 0
    lax.fori_loop(0, n_grp, out_wait, 0)
    if first:
        def count_drain(k, _):
            count_copy(k, False).wait_send()
            return 0
        lax.fori_loop(1, n_dev, count_drain, 0)


def router_rows(x, wr, lane, n_dev):
    lg = dot(x, wr[...])
    lg = jnp.where(lane < n_dev, lg[:, :LANES] + lg[:, LANES:], -1e30)
    mx = jnp.max(lg, axis=1, keepdims=True)
    ex = jnp.exp(lg - mx)
    sm = jnp.sum(ex, axis=1, keepdims=True)
    return ex / sm, mx + jnp.log(sm)


def base_grad(p, lz, v, zc):
    spread = jnp.sum(p * v, axis=1, keepdims=True)
    return p * (v - spread) + (zc * lz) * p


def split_rows(dl):
    hi = dl.astype(BF)
    lo = (dl - hi.astype(F32)).astype(BF)
    dl2 = jnp.concatenate([hi, lo], axis=1)
    return dl2, jnp.concatenate([dl2, hi], axis=1)


def expert_call(cfg, *args):
    n_dev, hd, cap, d, ff, ft, total_tok, first = cfg
    sd = jax.ShapeDtypeStruct
    rows = 2 * cap
    dma = pltpu.SemaphoreType.DMA
    scratch = [pltpu.VMEM((hd, cap, d), BF), pltpu.VMEM((hd, cap, d), BF), pltpu.VMEM((d, ff), F32),
               pltpu.VMEM((rows, d), F32), pltpu.VMEM((rows, d), F32), pltpu.VMEM((rows, d), F32),
               pltpu.VMEM((rows, d), BF), pltpu.VMEM((d, rows), BF), pltpu.VMEM((d, rows), BF),
               pltpu.VMEM((hd, cap, d), BF), dma((2,)), dma((2, hd)), dma((2, hd)), dma((hd // 2,))]
    out_shape = [sd((hd, cap, d), BF), sd((d, ff), F32), sd((ff, d), F32), sd((d, LANES), F32)]
    out_specs = [HBM, VM, VM, VM]
    if first:
        out_shape.append(sd((8, LANES), F32))
        out_specs.append(VM)
        scratch = [pltpu.VMEM((n_dev, 8, LANES), F32), dma((n_dev,)), dma((n_dev,))] + scratch
    return pl.pallas_call(
        functools.partial(expert_kernel, cfg), out_shape=out_shape, in_specs=[VM, HBM, HBM, VM, VM, VM, VM],
        out_specs=out_specs, scratch_shapes=scratch, name='expert_own' if first else 'expert_mirror',
        cost_estimate=pl.CostEstimate(flops=12 * hd * cap * d * ff, bytes_accessed=32 * 2 ** 20, transcendentals=0),
        compiler_params=pltpu.CompilerParams(has_side_effects=True, vmem_limit_bytes=VMEM_LIMIT))(*args)


def return_kernel(hd, go, gm, bo, bm, loc_sem, send_sem, recv_sem):
    me = lax.axis_index('ep')
    half = me // hd
    rank = lax.rem(me, hd)
    chip = rank // 2
    core = lax.rem(rank, 2)

    def peer_of(j, c):
        return xor3(chip, j) * 2 + lax.rem(core + c, 2)

    def row_copy(a, peer, slot):
        src, dst = ((go, bo), (gm, bm))[a]
        return pltpu.make_async_remote_copy(
            src_ref=src.at[peer], dst_ref=dst.at[slot], send_sem=send_sem.at[a, peer],
            recv_sem=recv_sem.at[a, slot], device_id=(half * hd + peer,), device_id_type=MESH_ID)

    own = [pltpu.make_async_copy(s.at[rank], t.at[rank], loc_sem.at[a]) for a, (s, t) in enumerate(((go, bo), (gm, bm)))]

    def start(peer):
        for a in (0, 1):
            row_copy(a, peer, rank).start()

    def wait(peer):
        for a in (0, 1):
            row_copy(a, peer, peer).wait_send()
            row_copy(a, peer, peer).wait_recv()

    def each(fn):
        fn(peer_of(0, 1))

        def body(j, _):
            fn(peer_of(j, 0))
            fn(peer_of(j, 1))
            return 0
        lax.fori_loop(1, hd // 2, body, 0)
    each(start)
    for c in own:
        c.start()
    for c in own:
        c.wait()
    each(wait)


def return_call(go, gm):
    hd = go.shape[0]
    dma = pltpu.SemaphoreType.DMA
    sd = jax.ShapeDtypeStruct(go.shape, BF)
    return pl.pallas_call(
        functools.partial(return_kernel, hd), out_shape=[sd, sd], in_specs=[HBM, HBM], out_specs=[HBM, HBM],
        scratch_shapes=[dma((2,)), dma((2, hd)), dma((2, hd))], name='row_return',
        cost_estimate=pl.CostEstimate(flops=10 ** 10, bytes_accessed=32 * 2 ** 20, transcendentals=0),
        compiler_params=pltpu.CompilerParams(has_side_effects=True))(go, gm)


def route_kernel(ne, cap, half_ref, idx_ref, slot_ref, cnt_ref, hot, cum):
    nb = idx_ref.shape[0]
    expert = lax.broadcasted_iota(jnp.int32, (ne, LANES), 0)
    shift = half_ref[0] * (ne // 2)
    for b in range(nb):
        hot[b * ne:(b + 1) * ne, :] = (expert == idx_ref[b:b + 1, :]).astype(F32)
    r = lax.broadcasted_iota(jnp.int32, (LANES, 2 * LANES), 0)
    c = lax.broadcasted_iota(jnp.int32, (LANES, 2 * LANES), 1)
    tri = ((r <= c) | (c >= LANES)).astype(F32).astype(BF)
    cum[...] = dot(hot[...].astype(BF), tri)
    carry = jnp.zeros((ne, LANES), F32)
    for b in range(nb):
        block = cum[b * ne:(b + 1) * ne, :]
        pos = jnp.sum(hot[b * ne:(b + 1) * ne, :] * (block[:, :LANES] + carry), axis=0, keepdims=True) - 1.0
        pos = pos.astype(jnp.int32)
        rel = idx_ref[b:b + 1, :] + shift
        rel = jnp.where(rel >= ne, rel - ne, rel)
        slot_ref[b:b + 1, :] = jnp.where(pos < cap, rel * cap + pos, ne * cap)
        carry = carry + block[:, LANES:]
    full = jnp.concatenate([carry, jnp.zeros((LANES - ne, LANES), F32)], axis=0)
    cnt_ref[...] = full.T[0:8, :]


def route_call(half, idx, ne, cap):
    nb = idx.shape[0] // LANES
    sd = jax.ShapeDtypeStruct
    return pl.pallas_call(
        functools.partial(route_kernel, ne, cap), out_shape=[sd((nb, LANES), jnp.int32), sd((8, LANES), F32)],
        in_specs=[SM, VM], out_specs=[VM, VM],
        scratch_shapes=[pltpu.VMEM((nb * ne, LANES), F32), pltpu.VMEM((nb * ne, 2 * LANES), F32)], name='route',
        compiler_params=pltpu.CompilerParams(vmem_limit_bytes=VMEM_LIMIT))(half, idx.reshape(nb, LANES))


def dispatch_kernel(nb, tb, ne, cap, d, slot_ref, cnt_ref, x_ref, dy_ref, sx_ref, sdy_ref, tmp, big):
    i = pl.program_id(0)
    nk = d // LANES

    @pl.when(i < nb)
    def _():
        xf = x_ref[...].astype(F32)
        df = dy_ref[...].astype(F32)
        for k in range(nk):
            tmp[pl.ds(k, tb, stride=8), :] = xf[:, k * LANES:(k + 1) * LANES]
            tmp[pl.ds(4 + k, tb, stride=8), :] = df[:, k * LANES:(k + 1) * LANES]

        def place(q, _):
            row = i * (tb // LANES) + q // (LANES // 16)
            col = lax.rem(q, LANES // 16) * 16
            for u in range(16):
                s = slot_ref[row, col + u]
                big[pl.ds(pl.multiple_of(s * 8, 8), 8), :] = tmp[pl.ds(pl.multiple_of((q * 16 + u) * 8, 8), 8), :]
            return 0
        lax.fori_loop(0, tb // 16, place, 0)

    @pl.when(i >= nb)
    def _():
        e = i - nb
        n = cnt_ref[e]
        ok = lax.broadcasted_iota(jnp.int32, (cap, LANES), 0) < n
        base = e * (cap * 8)
        for k in range(nk):
            xk = big[pl.ds(base + k, cap, stride=8), :]
            sx_ref[0, :, k * LANES:(k + 1) * LANES] = jnp.where(ok, xk, 0.0).astype(BF)
            dk = big[pl.ds(base + 4 + k, cap, stride=8), :]
            sdy_ref[0, :, k * LANES:(k + 1) * LANES] = jnp.where(ok, dk, 0.0).astype(BF)


def dispatch_call(slot, cnt, x, dy, ne, cap):
    t, d = x.shape
    tb = 512
    nb = t // tb
    sd = jax.ShapeDtypeStruct((ne, cap, d), BF)
    tok = pl.BlockSpec((tb, d), lambda i: (jnp.minimum(i, nb - 1), 0))
    out = pl.BlockSpec((1, cap, d), lambda i: (jnp.maximum(i - nb, 0), 0, 0))
    return pl.pallas_call(
        functools.partial(dispatch_kernel, nb, tb, ne, cap, d), grid=(nb + ne,), out_shape=[sd, sd],
        in_specs=[SM, SM, tok, tok], out_specs=[out, out],
        scratch_shapes=[pltpu.VMEM((tb * 8, LANES), F32), pltpu.VMEM((ne * cap * 8 + 8, LANES), F32)], name='dispatch',
        compiler_params=pltpu.CompilerParams(vmem_limit_bytes=VMEM_LIMIT))(slot, cnt, x, dy)


def combine_kernel(cfg, slot_ref, tot_ref, bo, bm, x_ref, wr, wrt, gx_ref, gwr, stat, tmp, big):
    nb, tb, n_dev, hd, cap, d, total_tok = cfg
    i = pl.program_id(0)
    nk = d // LANES

    def put(rows, e):
        f = rows.astype(F32)
        base = e * (cap * 8)
        for k in range(nk):
            big[pl.ds(base + k, cap, stride=8), :] = f[:, k * LANES:(k + 1) * LANES]
        big[pl.ds(base + nk, cap, stride=8), :] = jnp.zeros((cap, LANES), F32)

    @pl.when(i == 0)
    def _():
        big[n_dev * cap * 8:n_dev * cap * 8 + 8, :] = jnp.ones((8, LANES), F32)
        gwr[...] = jnp.zeros_like(gwr)
        stat[...] = jnp.zeros_like(stat)

    @pl.when(i < hd)
    def _():
        put(bo[0], i)

    @pl.when((i >= hd) & (i < n_dev))
    def _():
        put(bm[0], i)

    @pl.when(i >= n_dev)
    def _():
        b = i - n_dev

        def fetch(q, _):
            row = b * (tb // LANES) + q // (LANES // 16)
            col = lax.rem(q, LANES // 16) * 16
            for u in range(16):
                s = slot_ref[row, col + u]
                tmp[pl.ds(pl.multiple_of((q * 16 + u) * 8, 8), 8), :] = big[pl.ds(pl.multiple_of(s * 8, 8), 8), :]
            return 0
        lax.fori_loop(0, tb // 16, fetch, 0)
        x = x_ref[...]
        lane = lax.broadcasted_iota(jnp.int32, (tb, LANES), 1)
        p, lz = router_rows(x, wr, lane, n_dev)
        v = tot_ref[0:1, :] * (AUX_WEIGHT * n_dev / (float(total_tok) * total_tok))
        dl = base_grad(p, lz, v, 2.0 * Z_WEIGHT / total_tok)
        _, dl3 = split_rows(dl)
        gxd = dot(dl3, wrt[...])
        drop = tmp[pl.ds(nk, tb, stride=8), :]
        dl2, _ = split_rows(dl * drop)
        gw = lax.dot_general(x, dl2, (((0,), (0,)), ((), ())), preferred_element_type=F32)
        gwr[...] += gw[:, :LANES] + gw[:, LANES:]
        stat[0:1, :] += jnp.sum(p, axis=0, keepdims=True)
        stat[1:2, :] += jnp.sum(jnp.broadcast_to(lz * lz, (tb, LANES)), axis=0, keepdims=True)
        for k in range(nk):
            got = tmp[pl.ds(k, tb, stride=8), :]
            gx_ref[:, k * LANES:(k + 1) * LANES] = jnp.where(drop > 0.5, gxd[:, k * LANES:(k + 1) * LANES], got).astype(BF)


def combine_call(slot, tot, bo, bm, x, wr, wrt, total_tok):
    t, d = x.shape
    hd, cap, _ = bo.shape
    n_dev = 2 * hd
    tb = 512
    nb = t // tb
    sd = jax.ShapeDtypeStruct
    tok = pl.BlockSpec((tb, d), lambda i: (jnp.maximum(i - n_dev, 0), 0))
    const = lambda s: pl.BlockSpec(s, lambda i: (0, 0))
    return pl.pallas_call(
        functools.partial(combine_kernel, (nb, tb, n_dev, hd, cap, d, total_tok)), grid=(n_dev + nb,),
        out_shape=[sd((t, d), BF), sd((d, LANES), F32), sd((8, LANES), F32)],
        in_specs=[SM, VM, pl.BlockSpec((1, cap, d), lambda i: (jnp.minimum(i, hd - 1), 0, 0)),
                  pl.BlockSpec((1, cap, d), lambda i: (jnp.clip(i - hd, 0, hd - 1), 0, 0)), tok, VM, VM],
        out_specs=[tok, const((d, LANES)), const((8, LANES))],
        scratch_shapes=[pltpu.VMEM((tb * 8, LANES), F32), pltpu.VMEM((n_dev * cap * 8 + 8, LANES), F32)], name='combine',
        compiler_params=pltpu.CompilerParams(vmem_limit_bytes=VMEM_LIMIT))(slot, tot, bo, bm, x, wr, wrt)


def split_router(w_router):
    d, ne = w_router.shape
    hi = lax.reduce_precision(w_router, 8, 7)
    lo = lax.reduce_precision(w_router - hi, 8, 7)
    pad = lambda a: jnp.pad(a, ((0, 0), (0, LANES - ne)))
    wr = jnp.concatenate([pad(hi), pad(lo)], axis=1).astype(BF)
    wrt = jnp.concatenate([pad(hi), pad(hi), pad(lo)], axis=1).T.astype(BF)
    return wr, wrt


def solution(mesh):
    n_dev = mesh.shape['ep']
    hd = n_dev // 2
    mirror = [(i, (i + hd) % n_dev) for i in range(n_dev)]

    def expert_layer(x_tokens, w_router, expert_idx, w_in, w_out, grad_y):
        tokens, d_model = x_tokens.shape
        ff = w_in.shape[-1]
        ne = n_dev
        capacity = (5 * tokens + 4 * ne - 1) // (4 * ne)
        total_tok = tokens * n_dev
        me = lax.axis_index('ep')
        half = me // hd
        w_in_o, w_out_o = w_in[0], w_out[0]
        w_in_m = lax.ppermute(w_in_o, 'ep', mirror)
        w_out_m = lax.ppermute(w_out_o, 'ep', mirror)
        wr, wrt = split_router(w_router)

        slot, cnt = route_call(half.reshape(1).astype(jnp.int32), expert_idx, ne, capacity)
        own = cnt[0, :ne].astype(jnp.int32)
        rel_cnt = jnp.where(half == 0, own, jnp.roll(own, hd))
        sx, sdy = dispatch_call(slot, rel_cnt, x_tokens, grad_y, ne, capacity)
        base = (n_dev, hd, capacity, d_model, ff, 512, total_tok)
        gx_o, gwi_o, gwo_o, gwr_o, tot = expert_call(base + (True,), cnt, sx, sdy, w_in_o, w_out_o, wr, wrt)
        gx_m, gwi_m, gwo_m, gwr_m = expert_call(base + (False,), tot, sx, sdy, w_in_m, w_out_m, wr, wrt)
        gwi_r = lax.ppermute(gwi_m, 'ep', mirror)
        gwo_r = lax.ppermute(gwo_m, 'ep', mirror)
        back_o, back_m = return_call(gx_o, gx_m)
        grad_x, gwr_d, stat = combine_call(slot, tot, back_o, back_m, x_tokens, wr, wrt, total_tok)

        fin = jnp.concatenate([(gwr_d + gwr_m + gwr_o)[:, :ne].reshape(-1), stat[0, :ne], stat[1, :1]])
        fin = lax.psum(fin, 'ep')
        nr = d_model * ne
        grad_w_router = fin[:nr].reshape(d_model, ne)
        aux_loss = AUX_WEIGHT * ne * jnp.sum(tot[0, :ne] / total_tok * fin[nr:nr + ne] / total_tok)
        z_loss = Z_WEIGHT * fin[nr + ne] / total_tok
        return grad_x, (gwi_o + gwi_r)[None], (gwo_o + gwo_r)[None], grad_w_router, aux_loss, z_loss

    return jax.shard_map(expert_layer, mesh=mesh,
                         in_specs=(P('ep', None), P(None, None), P('ep'), P('ep', None, None), P('ep', None, None), P('ep', None)),
                         out_specs=(P('ep', None), P('ep', None, None), P('ep', None, None), P(None, None), P(), P()),
                         check_vma=False)
```

```python
import functools
import jax
import jax.numpy as jnp
from jax import lax
from jax.experimental import pallas as pl
from jax.experimental.pallas import tpu as pltpu
from jax.sharding import PartitionSpec as P

AUX_WEIGHT = 0.01
Z_WEIGHT = 0.001
BF = jnp.bfloat16
F32 = jnp.float32
LANES = 128
MESH_ID = pl.DeviceIdType.MESH
VMEM_LIMIT = 60 * 1024 * 1024
UNROLL = 32
SLAB = 4
VM = pl.BlockSpec(memory_space=pltpu.VMEM)
SM = pl.BlockSpec(memory_space=pltpu.SMEM)
HBM = pl.BlockSpec(memory_space=pltpu.HBM)


def xor3(a, b):
    out = 0
    for k in (1, 2, 4):
        out = out + k * lax.rem(a // k + b // k, 2)
    return out


def hop(i):
    odd = lax.rem(i, 2)
    j = (1 - odd) * (7 - i // 2) + odd * ((i + 1) // 2)
    return j - 7 * (1 - (i + 7) // 8) + 3 * (i // 7)


def dot(a, b, ca=1, cb=0):
    return lax.dot_general(a, b, (((ca,), (cb,)), ((), ())), preferred_element_type=F32)


def expert_kernel(cfg, *refs):
    n_dev, hd, cap, d, ff, ft, total_tok, first = cfg
    lead, sx, sdy, wi, wo, wr, wrt, gx_out, gwi, gwo, gwr = refs[:11]
    rest = refs[11:]
    if first:
        tot_ref, cbuf, csend, crecv = rest[0], *rest[1:4]
        rest = rest[4:]
    xr, dyr, gwot, dlw, oacc, dracc, gb, xt, gt, stage, loc_sem, send_sem, recv_sem, out_sem = rest
    me = lax.axis_index('ep')
    half = me // hd
    rank = lax.rem(me, hd)
    chip = rank // 2
    core = lax.rem(rank, 2)
    n_grp = hd // 2
    rows = 2 * cap
    off = 0 if first else hd

    def peer_of(j, c):
        return xor3(chip, hop(j)) * 2 + lax.rem(core + c, 2)

    def token_copy(a, src, dst, peer, slot):
        return pltpu.make_async_remote_copy(
            src_ref=src.at[off + peer], dst_ref=dst.at[slot], send_sem=send_sem.at[a, peer],
            recv_sem=recv_sem.at[a, slot], device_id=(half * hd + peer,), device_id_type=MESH_ID)

    if first:
        def count_copy(k, sending):
            peer = lax.rem(me + k, n_dev)
            slot = me if sending else peer
            return pltpu.make_async_remote_copy(
                src_ref=lead, dst_ref=cbuf.at[slot], send_sem=csend.at[peer],
                recv_sem=crecv.at[slot], device_id=(peer,), device_id_type=MESH_ID)

        def start_count(k, _):
            count_copy(k, True).start()
            return 0
        lax.fori_loop(1, n_dev, start_count, 0)
        cbuf[me] = lead[...]

    own_x = pltpu.make_async_copy(sx.at[off + rank], xr.at[rank], loc_sem.at[0])
    own_dy = pltpu.make_async_copy(sdy.at[off + rank], dyr.at[rank], loc_sem.at[1])
    own_x.start()
    own_dy.start()

    def start_peer(peer):
        token_copy(0, sx, xr, peer, rank).start()
        token_copy(1, sdy, dyr, peer, rank).start()

    start_peer(rank + 1 - 2 * core)

    def start_group(j, _):
        start_peer(peer_of(j, 0))
        start_peer(peer_of(j, 1))
        return 0
    lax.fori_loop(1, n_grp, start_group, 0)

    gwi[...] = jnp.zeros_like(gwi)
    gwot[...] = jnp.zeros_like(gwot)
    gwr[...] = jnp.zeros_like(gwr)

    if first:
        def wait_count(k, _):
            count_copy(k, False).wait_recv()
            return 0
        lax.fori_loop(1, n_dev, wait_count, 0)
        tot_ref[...] = jnp.sum(cbuf[...], axis=0)
        tot = tot_ref[0:1, :]
        e_id = me
    else:
        tot = lead[0:1, :]
        e_id = lax.rem(me + hd, n_dev)
    v = tot * (AUX_WEIGHT * n_dev / (float(total_tok) * total_tok))
    zc = 2.0 * Z_WEIGHT / total_tok

    def recv_wait(peer):
        token_copy(0, sx, xr, peer, peer).wait_recv()
        token_copy(1, sdy, dyr, peer, peer).wait_recv()

    def group(j, _):
        @pl.when(j == 0)
        def _():
            own_x.wait()
            own_dy.wait()

        @pl.when(j > 0)
        def _():
            recv_wait(peer_of(j, 0))
        recv_wait(peer_of(j, 1))
        pair = xor3(chip, hop(j))
        x = xr[pl.ds(2 * pair, 2)].reshape(rows, d)
        dyf = dyr[pl.ds(2 * pair, 2)].reshape(rows, d).astype(F32)
        lane = lax.broadcasted_iota(jnp.int32, (rows, LANES), 1)
        p, lz = router_rows(x, wr, lane, n_dev)
        hot = (lane == e_id).astype(F32)
        gate = jnp.sum(p * hot, axis=1, keepdims=True)
        g = (gate * dyf).astype(BF)
        gb[...] = g
        xt[...] = x.T
        gt[...] = g.T
        oacc[...] = jnp.zeros_like(oacc)
        dracc[...] = jnp.zeros_like(dracc)

        def ff_tile(f, _):
            fo = pl.multiple_of(f * ft, ft)
            wit = wi[:, pl.ds(fo, ft)]
            wot = wo[pl.ds(fo, ft), :]
            xx = xr[pl.ds(2 * pair, 2)].reshape(rows, d)
            h = jnp.maximum(dot(xx, wit), 0.0).astype(BF)
            oacc[...] += dot(h, wot)
            dh = dot(gb[...], wot, 1, 1)
            da = jnp.where(h > 0, dh, 0.0).astype(BF)
            dracc[...] += dot(da, wit, 1, 1)
            gwot[:, pl.ds(fo, ft)] += dot(gt[...], h)
            gwi[:, pl.ds(fo, ft)] += dot(xt[...], da)
            return 0
        lax.fori_loop(0, ff // ft, ff_tile, 0)

        o = oacc[...].astype(BF).astype(F32)
        dgate = jnp.sum(o * dyf, axis=1, keepdims=True)
        dl = (gate * dgate) * (hot - p) + base_grad(p, lz, v, zc)
        dl2, dl3 = split_rows(dl)
        dlw[...] = dot(dl3, wrt[...])
        gw = dot(xt[...], dl2)
        gwr[...] += gw[:, :LANES] + gw[:, LANES:]
        gx = (dracc[...].astype(BF).astype(F32) + dlw[...]).astype(BF)
        stage[pl.ds(2 * pair, 2)] = gx.reshape(2, cap, d)
        pltpu.make_async_copy(stage.at[pl.ds(2 * pair, 2)], gx_out.at[pl.ds(2 * pair, 2)], out_sem.at[pair]).start()
        return 0
    lax.fori_loop(0, n_grp, group, 0)

    def finish(f, _):
        fo = pl.multiple_of(f * ft, ft)
        gwo[pl.ds(fo, ft), :] = gwot[:, pl.ds(fo, ft)].T
        return 0
    lax.fori_loop(0, ff // ft, finish, 0)

    def send_wait(peer):
        token_copy(0, sx, xr, peer, peer).wait_send()
        token_copy(1, sdy, dyr, peer, peer).wait_send()

    send_wait(rank + 1 - 2 * core)

    def drain(j, _):
        send_wait(peer_of(j, 0))
        send_wait(peer_of(j, 1))
        return 0
    lax.fori_loop(1, n_grp, drain, 0)

    def out_wait(s, _):
        pltpu.make_async_copy(stage.at[pl.ds(2 * s, 2)], gx_out.at[pl.ds(2 * s, 2)], out_sem.at[s]).wait()
        return 0
    lax.fori_loop(0, n_grp, out_wait, 0)
    if first:
        def count_drain(k, _):
            count_copy(k, False).wait_send()
            return 0
        lax.fori_loop(1, n_dev, count_drain, 0)


def router_rows(x, wr, lane, n_dev):
    lg = dot(x, wr[...])
    lg = jnp.where(lane < n_dev, lg[:, :LANES] + lg[:, LANES:], -1e30)
    mx = jnp.max(lg, axis=1, keepdims=True)
    ex = jnp.exp(lg - mx)
    sm = jnp.sum(ex, axis=1, keepdims=True)
    return ex / sm, mx + jnp.log(sm)


def base_grad(p, lz, v, zc):
    spread = jnp.sum(p * v, axis=1, keepdims=True)
    return p * (v - spread) + (zc * lz) * p


def split_rows(dl):
    hi = dl.astype(BF)
    lo = (dl - hi.astype(F32)).astype(BF)
    dl2 = jnp.concatenate([hi, lo], axis=1)
    return dl2, jnp.concatenate([dl2, hi], axis=1)


def expert_call(cfg, *args):
    n_dev, hd, cap, d, ff, ft, total_tok, first = cfg
    sd = jax.ShapeDtypeStruct
    rows = 2 * cap
    dma = pltpu.SemaphoreType.DMA
    scratch = [pltpu.VMEM((hd, cap, d), BF), pltpu.VMEM((hd, cap, d), BF), pltpu.VMEM((d, ff), F32),
               pltpu.VMEM((rows, d), F32), pltpu.VMEM((rows, d), F32), pltpu.VMEM((rows, d), F32),
               pltpu.VMEM((rows, d), BF), pltpu.VMEM((d, rows), BF), pltpu.VMEM((d, rows), BF),
               pltpu.VMEM((hd, cap, d), BF), dma((2,)), dma((2, hd)), dma((2, hd)), dma((hd // 2,))]
    out_shape = [sd((hd, cap, d), BF), sd((d, ff), F32), sd((ff, d), F32), sd((d, LANES), F32)]
    out_specs = [HBM, VM, VM, VM]
    if first:
        out_shape.append(sd((8, LANES), F32))
        out_specs.append(VM)
        scratch = [pltpu.VMEM((n_dev, 8, LANES), F32), dma((n_dev,)), dma((n_dev,))] + scratch
    return pl.pallas_call(
        functools.partial(expert_kernel, cfg), out_shape=out_shape, in_specs=[VM, HBM, HBM, VM, VM, VM, VM],
        out_specs=out_specs, scratch_shapes=scratch, name='expert_own' if first else 'expert_mirror',
        cost_estimate=pl.CostEstimate(flops=12 * hd * cap * d * ff, bytes_accessed=32 * 2 ** 20, transcendentals=0),
        compiler_params=pltpu.CompilerParams(has_side_effects=True, vmem_limit_bytes=VMEM_LIMIT))(*args)


def return_kernel(cfg, go, gm, x_ref, slot, tot_ref, wr, wrt, gwr_o, gwr_m, bo, bm, gxd_ref, fin,
                  acc, part, red, loc_sem, send_sem, recv_sem, rs_send, rs_recv, ag_send, ag_recv):
    hd, n_dev, cap, tb, total_tok = cfg
    me = lax.axis_index('ep')
    half = me // hd
    rank = lax.rem(me, hd)
    chip = rank // 2
    core = lax.rem(rank, 2)
    t, d = x_ref.shape
    nk = d // LANES

    def peer_of(j, c):
        return xor3(chip, hop(j)) * 2 + lax.rem(core + c, 2)

    def row_copy(a, peer, slot):
        src, dst = ((go, bo), (gm, bm))[a]
        return pltpu.make_async_remote_copy(
            src_ref=src.at[peer], dst_ref=dst.at[slot], send_sem=send_sem.at[a, peer],
            recv_sem=recv_sem.at[a, slot], device_id=(half * hd + peer,), device_id_type=MESH_ID)

    own = [pltpu.make_async_copy(s.at[rank], t.at[rank], loc_sem.at[a]) for a, (s, t) in enumerate(((go, bo), (gm, bm)))]

    def start(peer):
        for a in (0, 1):
            row_copy(a, peer, rank).start()

    def wait(peer):
        for a in (0, 1):
            row_copy(a, peer, peer).wait_send()
            row_copy(a, peer, peer).wait_recv()

    def each(fn):
        fn(rank + 1 - 2 * core)

        def body(j, _):
            fn(peer_of(j, 0))
            fn(peer_of(j, 1))
            return 0
        lax.fori_loop(1, hd // 2, body, 0)
    each(start)
    for c in own:
        c.start()

    v = tot_ref[0:1, :] * (AUX_WEIGHT * n_dev / (float(total_tok) * total_tok))
    acc[...] = gwr_o[...] + gwr_m[...]
    red[...] = jnp.zeros_like(red)

    def block(b, _):
        at = pl.ds(pl.multiple_of(b * tb, tb), tb)
        x = x_ref[at, :]
        lane = lax.broadcasted_iota(jnp.int32, (tb, LANES), 1)
        p, lz = router_rows(x, wr, lane, n_dev)
        dl = base_grad(p, lz, v, 2.0 * Z_WEIGHT / total_tok)
        dl2, dl3 = split_rows(dl)
        gxd_ref[at, :] = dot(dl3, wrt[...]).astype(BF)
        drop = (slot[pl.ds(b, 1), :] >= n_dev * cap).astype(F32)
        drop = jnp.broadcast_to(drop, (LANES, LANES)).T.astype(BF)
        gw = dot(x.T, dl2 * jnp.concatenate([drop, drop], axis=1))
        acc[...] += gw[:, :LANES] + gw[:, LANES:]
        red[0:1, :] += jnp.sum(p, axis=0, keepdims=True)
        red[1:2, :] += jnp.sum(jnp.broadcast_to(lz * lz, (tb, LANES)), axis=0, keepdims=True)
        return 0
    lax.fori_loop(0, t // tb, block, 0)

    gt = acc[...].T
    part[...] = jnp.zeros_like(part)
    for k in range(nk):
        part[pl.ds(k, n_dev, stride=8), :] = gt[0:n_dev, k * LANES:(k + 1) * LANES]
    for k in (0, 1):
        part[pl.ds(nk + k, n_dev, stride=8), :] = jnp.broadcast_to(red[k:k + 1, :], (n_dev, LANES))

    def tile(ref, i):
        return ref.at[pl.ds(pl.multiple_of(i * 8, 8), 8)]

    def rs_copy(k, slot):
        peer = lax.rem(me + k, n_dev)
        at = me if slot else peer
        return pltpu.make_async_remote_copy(
            src_ref=tile(part, peer), dst_ref=tile(fin, n_dev + at), send_sem=rs_send.at[peer],
            recv_sem=rs_recv.at[at], device_id=(peer,), device_id_type=MESH_ID)

    def ag_copy(k, slot):
        peer = lax.rem(me + k, n_dev)
        at = me if slot else peer
        return pltpu.make_async_remote_copy(
            src_ref=red, dst_ref=tile(fin, at), send_sem=ag_send.at[peer],
            recv_sem=ag_recv.at[at], device_id=(peer,), device_id_type=MESH_ID)

    def others(fn):
        def body(k, _):
            fn(k)
            return 0
        lax.fori_loop(1, n_dev, body, 0)
    others(lambda k: rs_copy(k, True).start())
    mine = pl.ds(pl.multiple_of(me * 8, 8), 8)
    red[...] = part[mine, :]

    def collect(k):
        rs_copy(k, False).wait_recv()
        src = lax.rem(me + k, n_dev)
        red[...] += fin[pl.ds(pl.multiple_of((n_dev + src) * 8, 8), 8), :]
    others(collect)
    others(lambda k: ag_copy(k, True).start())
    fin[mine, :] = red[...]
    others(lambda k: ag_copy(k, False).wait_recv())
    others(lambda k: rs_copy(k, False).wait_send())
    others(lambda k: ag_copy(k, False).wait_send())
    for c in own:
        c.wait()
    each(wait)


def return_call(go, gm, x, slot, tot, wr, wrt, gwr_o, gwr_m, total_tok):
    hd, cap, d = go.shape
    n_dev = 2 * hd
    dma = pltpu.SemaphoreType.DMA
    sd = jax.ShapeDtypeStruct
    row = sd(go.shape, BF)
    return pl.pallas_call(
        functools.partial(return_kernel, (hd, n_dev, cap, LANES, total_tok)),
        out_shape=[row, row, sd(x.shape, BF), sd((2 * n_dev * 8, LANES), F32)],
        in_specs=[HBM, HBM] + [VM] * 7, out_specs=[HBM, HBM, VM, VM],
        scratch_shapes=[pltpu.VMEM((d, LANES), F32), pltpu.VMEM((n_dev * 8, LANES), F32), pltpu.VMEM((8, LANES), F32),
                        dma((2,)), dma((2, hd)), dma((2, hd))] + [dma((n_dev,))] * 4, name='row_return',
        cost_estimate=pl.CostEstimate(flops=10 ** 10, bytes_accessed=32 * 2 ** 20, transcendentals=0),
        compiler_params=pltpu.CompilerParams(has_side_effects=True, vmem_limit_bytes=VMEM_LIMIT))(
            go, gm, x, slot, tot, wr, wrt, gwr_o, gwr_m)


def route_kernel(ne, cap, half_ref, idx_ref, slot_ref, cnt_ref, hot, cum):
    nb = idx_ref.shape[0]
    expert = lax.broadcasted_iota(jnp.int32, (ne, LANES), 0)
    shift = half_ref[0] * (ne // 2)
    for b in range(nb):
        hot[b * ne:(b + 1) * ne, :] = (expert == idx_ref[b:b + 1, :]).astype(F32)
    r = lax.broadcasted_iota(jnp.int32, (LANES, 2 * LANES), 0)
    c = lax.broadcasted_iota(jnp.int32, (LANES, 2 * LANES), 1)
    tri = ((r <= c) | (c >= LANES)).astype(F32).astype(BF)
    cum[...] = dot(hot[...].astype(BF), tri)
    carry = jnp.zeros((ne, LANES), F32)
    for b in range(nb):
        block = cum[b * ne:(b + 1) * ne, :]
        pos = jnp.sum(hot[b * ne:(b + 1) * ne, :] * (block[:, :LANES] + carry), axis=0, keepdims=True) - 1.0
        pos = pos.astype(jnp.int32)
        rel = idx_ref[b:b + 1, :] + shift
        rel = jnp.where(rel >= ne, rel - ne, rel)
        slot_ref[b:b + 1, :] = jnp.where(pos < cap, rel * cap + pos, ne * cap)
        carry = carry + block[:, LANES:]
    full = jnp.concatenate([carry, jnp.zeros((LANES - ne, LANES), F32)], axis=0)
    cnt_ref[...] = full.T[0:8, :]


def route_call(half, idx, ne, cap):
    nb = idx.shape[0] // LANES
    sd = jax.ShapeDtypeStruct
    return pl.pallas_call(
        functools.partial(route_kernel, ne, cap), out_shape=[sd((nb, LANES), jnp.int32), sd((8, LANES), F32)],
        in_specs=[SM, VM], out_specs=[VM, VM],
        scratch_shapes=[pltpu.VMEM((nb * ne, LANES), F32), pltpu.VMEM((nb * ne, 2 * LANES), F32)], name='route',
        compiler_params=pltpu.CompilerParams(vmem_limit_bytes=VMEM_LIMIT))(half, idx.reshape(nb, LANES))


def dispatch_kernel(nb, tb, ne, cap, d, slot_ref, cnt_ref, x_ref, dy_ref, sx_ref, sdy_ref, tmp, big):
    i = pl.program_id(0)
    nk = d // LANES

    @pl.when(i < nb)
    def _():
        xf = x_ref[...].astype(F32)
        df = dy_ref[...].astype(F32)
        for k in range(nk):
            tmp[pl.ds(k, tb, stride=8), :] = xf[:, k * LANES:(k + 1) * LANES]
            tmp[pl.ds(4 + k, tb, stride=8), :] = df[:, k * LANES:(k + 1) * LANES]

        def place(q, _):
            row = i * (tb // LANES) + q // (LANES // UNROLL)
            col = lax.rem(q, LANES // UNROLL) * UNROLL
            at = [slot_ref[row, col + u] * 8 for u in range(UNROLL)]
            rows = tmp[pl.ds(pl.multiple_of(q * (8 * UNROLL), 8), 8 * UNROLL), :]
            for u in range(UNROLL):
                big[pl.ds(pl.multiple_of(at[u], 8), 8), :] = rows[8 * u:8 * u + 8]
            return 0
        lax.fori_loop(0, tb // UNROLL, place, 0)

    @pl.when(i >= nb)
    def _():
        e = i - nb
        n = cnt_ref[e]
        ok = lax.broadcasted_iota(jnp.int32, (cap, LANES), 0) < n
        base = e * (cap * 8)
        for k in range(nk):
            xk = big[pl.ds(base + k, cap, stride=8), :]
            sx_ref[0, :, k * LANES:(k + 1) * LANES] = jnp.where(ok, xk, 0.0).astype(BF)
            dk = big[pl.ds(base + 4 + k, cap, stride=8), :]
            sdy_ref[0, :, k * LANES:(k + 1) * LANES] = jnp.where(ok, dk, 0.0).astype(BF)


def dispatch_call(slot, cnt, x, dy, ne, cap):
    t, d = x.shape
    tb = 512
    nb = t // tb
    sd = jax.ShapeDtypeStruct((ne, cap, d), BF)
    tok = pl.BlockSpec((tb, d), lambda i: (jnp.minimum(i, nb - 1), 0))
    out = pl.BlockSpec((1, cap, d), lambda i: (jnp.maximum(i - nb, 0), 0, 0))
    return pl.pallas_call(
        functools.partial(dispatch_kernel, nb, tb, ne, cap, d), grid=(nb + ne,), out_shape=[sd, sd],
        in_specs=[SM, SM, tok, tok], out_specs=[out, out],
        scratch_shapes=[pltpu.VMEM((tb * 8, LANES), F32), pltpu.VMEM((ne * cap * 8 + 8, LANES), F32)], name='dispatch',
        compiler_params=pltpu.CompilerParams(vmem_limit_bytes=VMEM_LIMIT))(slot, cnt, x, dy)


def combine_kernel(cfg, slot_ref, bo, bm, gxd, gx_ref, tmp, big):
    tb, n_dev, hd, cap, d = cfg
    i = pl.program_id(0)
    nk = d // LANES

    def put(rows, e):
        f = rows.astype(F32)
        base = e * (cap * SLAB)
        for k in range(nk):
            big[pl.ds(base + k, cap, stride=SLAB), :] = f[:, k * LANES:(k + 1) * LANES]
        big[pl.ds(base + nk, cap, stride=SLAB), :] = jnp.zeros((cap, LANES), F32)

    @pl.when(i == 0)
    def _():
        big[n_dev * cap * SLAB:n_dev * cap * SLAB + 8, :] = jnp.ones((8, LANES), F32)

    @pl.when(i < hd)
    def _():
        put(bo[0], i)

    @pl.when((i >= hd) & (i < n_dev))
    def _():
        put(bm[0], i)

    @pl.when(i >= n_dev)
    def _():
        b = i - n_dev

        def fetch(q, _):
            row = b * (tb // LANES) + q // (LANES // UNROLL)
            col = lax.rem(q, LANES // UNROLL) * UNROLL
            at = [slot_ref[row, col + u] * SLAB for u in range(UNROLL)]
            rows = [big[pl.ds(pl.multiple_of(at[u], SLAB), SLAB), :] for u in range(UNROLL)]
            tmp[pl.ds(pl.multiple_of(q * (SLAB * UNROLL), 8), SLAB * UNROLL), :] = jnp.concatenate(rows, axis=0)
            return 0
        lax.fori_loop(0, tb // UNROLL, fetch, 0)
        drop = tmp[pl.ds(nk, tb, stride=SLAB), :] > 0.5
        for k in range(nk):
            lanes = slice(k * LANES, (k + 1) * LANES)
            got = tmp[pl.ds(k, tb, stride=SLAB), :]
            gx_ref[:, lanes] = jnp.where(drop, gxd[:, lanes].astype(F32), got).astype(BF)


def combine_call(slot, bo, bm, gxd):
    t, d = gxd.shape
    hd, cap, _ = bo.shape
    n_dev = 2 * hd
    tb = 512
    tok = pl.BlockSpec((tb, d), lambda i: (jnp.maximum(i - n_dev, 0), 0))
    return pl.pallas_call(
        functools.partial(combine_kernel, (tb, n_dev, hd, cap, d)), grid=(n_dev + t // tb,),
        out_shape=jax.ShapeDtypeStruct((t, d), BF),
        in_specs=[SM, pl.BlockSpec((1, cap, d), lambda i: (jnp.minimum(i, hd - 1), 0, 0)),
                  pl.BlockSpec((1, cap, d), lambda i: (jnp.clip(i - hd, 0, hd - 1), 0, 0)), tok],
        out_specs=tok,
        scratch_shapes=[pltpu.VMEM((tb * SLAB, LANES), F32), pltpu.VMEM((n_dev * cap * SLAB + 8, LANES), F32)], name='combine',
        compiler_params=pltpu.CompilerParams(vmem_limit_bytes=VMEM_LIMIT))(slot, bo, bm, gxd)


def split_router(w_router):
    d, ne = w_router.shape
    hi = lax.reduce_precision(w_router, 8, 7)
    lo = lax.reduce_precision(w_router - hi, 8, 7)
    pad = lambda a: jnp.pad(a, ((0, 0), (0, LANES - ne)))
    wr = jnp.concatenate([pad(hi), pad(lo)], axis=1).astype(BF)
    wrt = jnp.concatenate([pad(hi), pad(hi), pad(lo)], axis=1).T.astype(BF)
    return wr, wrt


def solution(mesh):
    n_dev = mesh.shape['ep']
    hd = n_dev // 2
    mirror = [(i, (i + hd) % n_dev) for i in range(n_dev)]

    def expert_layer(x_tokens, w_router, expert_idx, w_in, w_out, grad_y):
        tokens, d_model = x_tokens.shape
        ff = w_in.shape[-1]
        ne = n_dev
        capacity = (5 * tokens + 4 * ne - 1) // (4 * ne)
        total_tok = tokens * n_dev
        me = lax.axis_index('ep')
        half = me // hd
        w_in_o, w_out_o = w_in[0], w_out[0]
        w_in_m = lax.ppermute(w_in_o, 'ep', mirror)
        w_out_m = lax.ppermute(w_out_o, 'ep', mirror)
        wr, wrt = split_router(w_router)

        slot, cnt = route_call(half.reshape(1).astype(jnp.int32), expert_idx, ne, capacity)
        own = cnt[0, :ne].astype(jnp.int32)
        rel_cnt = jnp.where(half == 0, own, jnp.roll(own, hd))
        sx, sdy = dispatch_call(slot, rel_cnt, x_tokens, grad_y, ne, capacity)
        base = (n_dev, hd, capacity, d_model, ff, 512, total_tok)
        gx_o, gwi_o, gwo_o, gwr_o, tot = expert_call(base + (True,), cnt, sx, sdy, w_in_o, w_out_o, wr, wrt)
        gx_m, gwi_m, gwo_m, gwr_m = expert_call(base + (False,), tot, sx, sdy, w_in_m, w_out_m, wr, wrt)
        gwi_r = lax.ppermute(gwi_m, 'ep', mirror)
        gwo_r = lax.ppermute(gwo_m, 'ep', mirror)
        back_o, back_m, gx_drop, fin = return_call(gx_o, gx_m, x_tokens, slot, tot, wr, wrt, gwr_o, gwr_m, total_tok)
        grad_x = combine_call(slot, back_o, back_m, gx_drop)
        fin = fin[:ne * 8].reshape(ne, 8, LANES)
        nk = d_model // LANES
        grad_w_router = fin[:, :nk].reshape(ne, d_model).T
        aux_loss = AUX_WEIGHT * ne * jnp.sum(tot[0, :ne] / total_tok * fin[0, nk, :ne] / total_tok)
        z_loss = Z_WEIGHT * fin[0, nk + 1, 0] / total_tok
        return grad_x, (gwi_o + gwi_r)[None], (gwo_o + gwo_r)[None], grad_w_router, aux_loss, z_loss

    return jax.shard_map(expert_layer, mesh=mesh,
                         in_specs=(P('ep', None), P(None, None), P('ep'), P('ep', None, None), P('ep', None, None), P('ep', None)),
                         out_specs=(P('ep', None), P('ep', None, None), P('ep', None, None), P(None, None), P(), P()),
                         check_vma=False)
```

```python
import functools
import jax
import jax.numpy as jnp
from jax import lax
from jax.experimental import pallas as pl
from jax.experimental.pallas import tpu as pltpu
from jax.sharding import PartitionSpec as P

AUX_WEIGHT = 0.01
Z_WEIGHT = 0.001
BF = jnp.bfloat16
F32 = jnp.float32
LANES = 128
MESH_ID = pl.DeviceIdType.MESH
VMEM_LIMIT = 60 * 1024 * 1024
UNROLL = 32
SLAB = 4
VM = pl.BlockSpec(memory_space=pltpu.VMEM)
SM = pl.BlockSpec(memory_space=pltpu.SMEM)
HBM = pl.BlockSpec(memory_space=pltpu.HBM)


def xor3(a, b):
    out = 0
    for k in (1, 2, 4):
        out = out + k * lax.rem(a // k + b // k, 2)
    return out


def hop(i):
    odd = lax.rem(i, 2)
    j = (1 - odd) * (7 - i // 2) + odd * ((i + 1) // 2)
    return j - 7 * (1 - (i + 7) // 8) + 3 * (i // 7)


def dot(a, b, ca=1, cb=0):
    return lax.dot_general(a, b, (((ca,), (cb,)), ((), ())), preferred_element_type=F32)


def expert_kernel(cfg, *refs):
    n_dev, hd, cap, d, ff, ft, total_tok = cfg
    (cnt_ref, sx, sdy, wi_o, wo_o, wi_m, wr, wrt,
     gx_out, gwi_o, gwo_o, gwi_m, gwo_m, gwr, tot_ref,
     cbuf, wo_m, xr, dyr, gwot, dlw, oacc, dracc, gb, xt, gt,
     csend, crecv, loc_sem, send_sem, recv_sem, out_sem, w_send, w_recv) = refs
    me = lax.axis_index('ep')
    half = me // hd
    rank = lax.rem(me, hd)
    chip = rank // 2
    core = lax.rem(rank, 2)
    n_grp = hd // 2
    rows = 2 * cap
    twin = rank + 1 - 2 * core
    mirror = lax.rem(me + hd, n_dev)

    def peer_of(j, c):
        return xor3(chip, hop(j)) * 2 + lax.rem(core + c, 2)

    def token_copy(part, a, peer, slot):
        src, dst = ((sx, xr), (sdy, dyr))[a]
        off = part * hd
        return pltpu.make_async_remote_copy(
            src_ref=src.at[off + peer], dst_ref=dst.at[off + slot], send_sem=send_sem.at[a, off + peer],
            recv_sem=recv_sem.at[a, off + slot], device_id=(half * hd + peer,), device_id_type=MESH_ID)

    def count_copy(k, sending):
        peer = lax.rem(me + k, n_dev)
        slot = me if sending else peer
        return pltpu.make_async_remote_copy(
            src_ref=cnt_ref, dst_ref=cbuf.at[slot], send_sem=csend.at[peer],
            recv_sem=crecv.at[slot], device_id=(peer,), device_id_type=MESH_ID)

    def others(fn):
        def body(k, _):
            fn(k)
            return 0
        lax.fori_loop(1, n_dev, body, 0)

    def each(fn):
        fn(twin)

        def body(j, _):
            fn(peer_of(j, 0))
            fn(peer_of(j, 1))
            return 0
        lax.fori_loop(1, n_grp, body, 0)

    weight = pltpu.make_async_remote_copy(src_ref=wo_o, dst_ref=wo_m, send_sem=w_send, recv_sem=w_recv,
                                          device_id=(mirror,), device_id_type=MESH_ID)
    others(lambda k: count_copy(k, True).start())
    cbuf[me] = cnt_ref[...]
    own = [pltpu.make_async_copy(src.at[q * hd + rank], dst.at[q * hd + rank], loc_sem.at[q, a])
           for q in (0, 1) for a, (src, dst) in enumerate(((sx, xr), (sdy, dyr)))]
    for c in own:
        c.start()

    def start(part):
        def one(peer):
            token_copy(part, 0, peer, rank).start()
            token_copy(part, 1, peer, rank).start()
        each(one)
    start(0)
    weight.start()
    start(1)

    gwr[...] = jnp.zeros_like(gwr)
    others(lambda k: count_copy(k, False).wait_recv())
    tot_ref[...] = jnp.sum(cbuf[...], axis=0)
    v = tot_ref[0:1, :] * (AUX_WEIGHT * n_dev / (float(total_tok) * total_tok))
    zc = 2.0 * Z_WEIGHT / total_tok

    for part, (e_id, wi, wo, gwi, gwo) in enumerate(((me, wi_o, wo_o, gwi_o, gwo_o), (mirror, wi_m, wo_m, gwi_m, gwo_m))):
        gwi[...] = jnp.zeros_like(gwi)
        gwot[...] = jnp.zeros_like(gwot)
        if part:
            weight.wait_recv()

        def recv_wait(peer):
            token_copy(part, 0, peer, peer).wait_recv()
            token_copy(part, 1, peer, peer).wait_recv()

        def group(j, _):
            @pl.when(j == 0)
            def _():
                own[2 * part].wait()
                own[2 * part + 1].wait()

            @pl.when(j > 0)
            def _():
                recv_wait(peer_of(j, 0))
            recv_wait(peer_of(j, 1))
            pair = part * n_grp + xor3(chip, hop(j))
            two = pl.ds(2 * pair, 2)
            x = xr[two].reshape(rows, d)
            dyf = dyr[two].reshape(rows, d).astype(F32)
            lane = lax.broadcasted_iota(jnp.int32, (rows, LANES), 1)
            p, lz = router_rows(x, wr, lane, n_dev)
            hot = (lane == e_id).astype(F32)
            gate = jnp.sum(p * hot, axis=1, keepdims=True)
            g = (gate * dyf).astype(BF)
            gb[...] = g
            xt[...] = x.T
            gt[...] = g.T
            oacc[...] = jnp.zeros_like(oacc)
            dracc[...] = jnp.zeros_like(dracc)

            def ff_tile(f, _):
                fo = pl.multiple_of(f * ft, ft)
                wit = wi[:, pl.ds(fo, ft)]
                wot = wo[pl.ds(fo, ft), :]
                xx = xr[two].reshape(rows, d)
                h = jnp.maximum(dot(xx, wit), 0.0).astype(BF)
                oacc[...] += dot(h, wot)
                dh = dot(gb[...], wot, 1, 1)
                da = jnp.where(h > 0, dh, 0.0).astype(BF)
                dracc[...] += dot(da, wit, 1, 1)
                gwot[:, pl.ds(fo, ft)] += dot(gt[...], h)
                gwi[:, pl.ds(fo, ft)] += dot(xt[...], da)
                return 0
            lax.fori_loop(0, ff // ft, ff_tile, 0)

            o = oacc[...].astype(BF).astype(F32)
            dgate = jnp.sum(o * dyr[two].reshape(rows, d).astype(F32), axis=1, keepdims=True)
            dl = (gate * dgate) * (hot - p) + base_grad(p, lz, v, zc)
            dl2, dl3 = split_rows(dl)
            dlw[...] = dot(dl3, wrt[...])
            gw = dot(xt[...], dl2)
            gwr[...] += gw[:, :LANES] + gw[:, LANES:]
            gx = (dracc[...].astype(BF).astype(F32) + dlw[...]).astype(BF)
            dyr[two] = gx.reshape(2, cap, d)
            pltpu.make_async_copy(dyr.at[two], gx_out.at[two], out_sem.at[pair]).start()
            return 0
        lax.fori_loop(0, n_grp, group, 0)

        def finish(f, _):
            fo = pl.multiple_of(f * ft, ft)
            gwo[pl.ds(fo, ft), :] = gwot[:, pl.ds(fo, ft)].T
            return 0
        lax.fori_loop(0, ff // ft, finish, 0)

    for part in (0, 1):
        def drain(peer):
            token_copy(part, 0, peer, peer).wait_send()
            token_copy(part, 1, peer, peer).wait_send()
        each(drain)
    weight.wait_send()

    def out_wait(s, _):
        pltpu.make_async_copy(dyr.at[pl.ds(2 * s, 2)], gx_out.at[pl.ds(2 * s, 2)], out_sem.at[s]).wait()
        return 0
    lax.fori_loop(0, 2 * n_grp, out_wait, 0)
    others(lambda k: count_copy(k, False).wait_send())


def router_rows(x, wr, lane, n_dev):
    lg = dot(x, wr[...])
    lg = jnp.where(lane < n_dev, lg[:, :LANES] + lg[:, LANES:], -1e30)
    mx = jnp.max(lg, axis=1, keepdims=True)
    ex = jnp.exp(lg - mx)
    sm = jnp.sum(ex, axis=1, keepdims=True)
    return ex / sm, mx + jnp.log(sm)


def base_grad(p, lz, v, zc):
    spread = jnp.sum(p * v, axis=1, keepdims=True)
    return p * (v - spread) + (zc * lz) * p


def split_rows(dl):
    hi = dl.astype(BF)
    lo = (dl - hi.astype(F32)).astype(BF)
    dl2 = jnp.concatenate([hi, lo], axis=1)
    return dl2, jnp.concatenate([dl2, hi], axis=1)


def expert_call(cfg, *args):
    n_dev, hd, cap, d, ff, ft, total_tok = cfg
    sd = jax.ShapeDtypeStruct
    rows = 2 * cap
    dma = pltpu.SemaphoreType.DMA
    vf = lambda *shape: pltpu.VMEM(shape, F32)
    vb = lambda *shape: pltpu.VMEM(shape, BF)
    scratch = [vf(n_dev, 8, LANES), vb(ff, d), vb(n_dev, cap, d), vb(n_dev, cap, d), vf(d, ff), vf(rows, d), vf(rows, d), vf(rows, d),
               vb(rows, d), vb(d, rows), vb(d, rows), dma((n_dev,)), dma((n_dev,)), dma((2, 2)), dma((2, n_dev)), dma((2, n_dev)),
               dma((hd,)), dma, dma]
    wi, wo = sd((d, ff), F32), sd((ff, d), F32)
    return pl.pallas_call(
        functools.partial(expert_kernel, cfg),
        out_shape=[sd((n_dev, cap, d), BF), wi, wo, wi, wo, sd((d, LANES), F32), sd((8, LANES), F32)],
        in_specs=[VM, HBM, HBM] + [VM] * 5, out_specs=[HBM] + [VM] * 6, scratch_shapes=scratch, name='experts',
        cost_estimate=pl.CostEstimate(flops=24 * hd * cap * d * ff, bytes_accessed=64 * 2 ** 20, transcendentals=0),
        compiler_params=pltpu.CompilerParams(has_side_effects=True, vmem_limit_bytes=VMEM_LIMIT))(*args)


def finish_kernel(cfg, slot_sm, rows, gwi, gwo, x_ref, slot, tot_ref, wr, wrt, gwr, gx_ref, gwi_r, gwo_r, fin,
                  bo, bm, big, tmp, acc, part, red, loc_sem, send_sem, recv_sem, rs_send, rs_recv, ag_send, ag_recv,
                  gr_send, gr_recv):
    hd, n_dev, cap, tb, total_tok = cfg
    me = lax.axis_index('ep')
    half = me // hd
    rank = lax.rem(me, hd)
    chip = rank // 2
    core = lax.rem(rank, 2)
    t, d = x_ref.shape
    nk = d // LANES

    def peer_of(j, c):
        return xor3(chip, hop(j)) * 2 + lax.rem(core + c, 2)

    def row_copy(a, peer, slot):
        dst = (bo, bm)[a]
        return pltpu.make_async_remote_copy(
            src_ref=rows.at[a * hd + peer], dst_ref=dst.at[slot], send_sem=send_sem.at[a, peer],
            recv_sem=recv_sem.at[a, slot], device_id=(half * hd + peer,), device_id_type=MESH_ID)

    own = [pltpu.make_async_copy(rows.at[a * hd + rank], b.at[rank], loc_sem.at[a]) for a, b in enumerate((bo, bm))]

    def grad_copy(a):
        src, dst = ((gwo, gwo_r), (gwi, gwi_r))[a]
        return pltpu.make_async_remote_copy(
            src_ref=src, dst_ref=dst, send_sem=gr_send.at[a], recv_sem=gr_recv.at[a],
            device_id=(lax.rem(me + hd, n_dev),), device_id_type=MESH_ID)

    def put(buf, base, s):
        f = buf[s].astype(F32)
        at = pl.ds((base + s) * cap, cap)
        for k in range(nk):
            big[at, k, :] = f[:, k * LANES:(k + 1) * LANES]
        big[at, nk, :] = jnp.zeros((cap, LANES), F32)

    def start(peer):
        for a in (0, 1):
            row_copy(a, peer, rank).start()

    def wait(peer):
        for a in (0, 1):
            row_copy(a, peer, peer).wait_recv()
            put((bo, bm)[a], a * hd, peer)

    def drain(peer):
        for a in (0, 1):
            row_copy(a, peer, peer).wait_send()

    def each(fn):
        fn(rank + 1 - 2 * core)

        def body(j, _):
            fn(peer_of(j, 0))
            fn(peer_of(j, 1))
            return 0
        lax.fori_loop(1, hd // 2, body, 0)
    each(start)
    grad_copy(0).start()
    for c in own:
        c.start()

    v = tot_ref[0:1, :] * (AUX_WEIGHT * n_dev / (float(total_tok) * total_tok))
    acc[...] = gwr[...]
    red[...] = jnp.zeros_like(red)

    def block(b, _):
        at = pl.ds(pl.multiple_of(b * tb, tb), tb)
        x = x_ref[at, :]
        lane = lax.broadcasted_iota(jnp.int32, (tb, LANES), 1)
        p, lz = router_rows(x, wr, lane, n_dev)
        dl = base_grad(p, lz, v, 2.0 * Z_WEIGHT / total_tok)
        dl2, dl3 = split_rows(dl)
        gx_ref[at, :] = dot(dl3, wrt[...]).astype(BF)
        drop = (slot[pl.ds(b, 1), :] >= n_dev * cap).astype(F32)
        drop = jnp.broadcast_to(drop, (LANES, LANES)).T.astype(BF)
        gw = dot(x.T, dl2 * jnp.concatenate([drop, drop], axis=1))
        acc[...] += gw[:, :LANES] + gw[:, LANES:]
        red[0:1, :] += jnp.sum(p, axis=0, keepdims=True)
        red[1:2, :] += jnp.sum(jnp.broadcast_to(lz * lz, (tb, LANES)), axis=0, keepdims=True)
        return 0
    lax.fori_loop(0, t // tb, block, 0)

    gt = acc[...].T
    part[...] = jnp.zeros_like(part)
    for k in range(nk):
        part[pl.ds(k, n_dev, stride=8), :] = gt[0:n_dev, k * LANES:(k + 1) * LANES]
    for k in (0, 1):
        part[pl.ds(nk + k, n_dev, stride=8), :] = jnp.broadcast_to(red[k:k + 1, :], (n_dev, LANES))

    def tile(ref, i):
        return ref.at[pl.ds(pl.multiple_of(i * 8, 8), 8)]

    def rs_copy(k, slot):
        peer = lax.rem(me + k, n_dev)
        at = me if slot else peer
        return pltpu.make_async_remote_copy(
            src_ref=tile(part, peer), dst_ref=tile(fin, n_dev + at), send_sem=rs_send.at[peer],
            recv_sem=rs_recv.at[at], device_id=(peer,), device_id_type=MESH_ID)

    def ag_copy(k, slot):
        peer = lax.rem(me + k, n_dev)
        at = me if slot else peer
        return pltpu.make_async_remote_copy(
            src_ref=red, dst_ref=tile(fin, at), send_sem=ag_send.at[peer],
            recv_sem=ag_recv.at[at], device_id=(peer,), device_id_type=MESH_ID)

    def others(fn):
        def body(k, _):
            fn(k)
            return 0
        lax.fori_loop(1, n_dev, body, 0)
    others(lambda k: rs_copy(k, True).start())
    grad_copy(1).start()
    for c in own:
        c.wait()
    put(bo, 0, rank)
    put(bm, hd, rank)
    big[n_dev * cap] = jnp.ones((SLAB, LANES), F32)
    each(wait)

    def combine(b, _):
        def fetch(q, _):
            rows = [big[slot_sm[b, q * UNROLL + u]] for u in range(UNROLL)]
            tmp[pl.ds(pl.multiple_of(q * (SLAB * UNROLL), 8), SLAB * UNROLL), :] = jnp.concatenate(rows, axis=0)
            return 0
        lax.fori_loop(0, LANES // UNROLL, fetch, 0)
        at = pl.ds(pl.multiple_of(b * LANES, LANES), LANES)
        drop = tmp[pl.ds(nk, LANES, stride=SLAB), :] > 0.5
        for k in range(nk):
            lanes = slice(k * LANES, (k + 1) * LANES)
            got = tmp[pl.ds(k, LANES, stride=SLAB), :]
            gx_ref[at, lanes] = jnp.where(drop, gx_ref[at, lanes].astype(F32), got).astype(BF)
        return 0
    lax.fori_loop(0, t // LANES, combine, 0)
    mine = pl.ds(pl.multiple_of(me * 8, 8), 8)
    red[...] = part[mine, :]

    def collect(k):
        rs_copy(k, False).wait_recv()
        src = lax.rem(me + k, n_dev)
        red[...] += fin[pl.ds(pl.multiple_of((n_dev + src) * 8, 8), 8), :]
    others(collect)
    others(lambda k: ag_copy(k, True).start())
    fin[mine, :] = red[...]
    others(lambda k: ag_copy(k, False).wait_recv())
    others(lambda k: rs_copy(k, False).wait_send())
    others(lambda k: ag_copy(k, False).wait_send())
    each(drain)
    for a in (0, 1):
        grad_copy(a).wait()


def finish_call(slot, gx, gwi, gwo, x, tot, wr, wrt, gwr, total_tok):
    n_dev, cap, d = gx.shape
    hd = n_dev // 2
    dma = pltpu.SemaphoreType.DMA
    sd = jax.ShapeDtypeStruct
    rows = pltpu.VMEM((hd, cap, d), BF)
    return pl.pallas_call(
        functools.partial(finish_kernel, (hd, n_dev, cap, LANES, total_tok)),
        out_shape=[sd(x.shape, BF), sd(gwi.shape, F32), sd(gwo.shape, F32), sd((2 * n_dev * 8, LANES), F32)],
        in_specs=[SM] + [HBM] * 3 + [VM] * 6, out_specs=[VM, HBM, HBM, VM],
        scratch_shapes=[rows, rows, pltpu.VMEM((n_dev * cap + 1, SLAB, LANES), F32), pltpu.VMEM((LANES * SLAB, LANES), F32),
                        pltpu.VMEM((d, LANES), F32), pltpu.VMEM((n_dev * 8, LANES), F32), pltpu.VMEM((8, LANES), F32),
                        dma((2,)), dma((2, hd)), dma((2, hd))] + [dma((n_dev,))] * 4 + [dma((2,))] * 2, name='finish',
        cost_estimate=pl.CostEstimate(flops=10 ** 10, bytes_accessed=32 * 2 ** 20, transcendentals=0),
        compiler_params=pltpu.CompilerParams(has_side_effects=True, vmem_limit_bytes=VMEM_LIMIT))(
            slot, gx, gwi, gwo, x, slot, tot, wr, wrt, gwr)


def route_kernel(ne, cap, half_ref, idx_ref, slot_ref, cnt_ref, hot, cum):
    nb = idx_ref.shape[0]
    expert = lax.broadcasted_iota(jnp.int32, (ne, LANES), 0)
    shift = half_ref[0] * (ne // 2)
    for b in range(nb):
        hot[b * ne:(b + 1) * ne, :] = (expert == idx_ref[b:b + 1, :]).astype(F32)
    r = lax.broadcasted_iota(jnp.int32, (LANES, 2 * LANES), 0)
    c = lax.broadcasted_iota(jnp.int32, (LANES, 2 * LANES), 1)
    tri = ((r <= c) | (c >= LANES)).astype(F32).astype(BF)
    cum[...] = dot(hot[...].astype(BF), tri)
    carry = jnp.zeros((ne, LANES), F32)
    for b in range(nb):
        block = cum[b * ne:(b + 1) * ne, :]
        pos = jnp.sum(hot[b * ne:(b + 1) * ne, :] * (block[:, :LANES] + carry), axis=0, keepdims=True) - 1.0
        pos = pos.astype(jnp.int32)
        rel = idx_ref[b:b + 1, :] + shift
        rel = jnp.where(rel >= ne, rel - ne, rel)
        slot_ref[b:b + 1, :] = jnp.where(pos < cap, rel * cap + pos, ne * cap)
        carry = carry + block[:, LANES:]
    full = jnp.concatenate([carry, jnp.zeros((LANES - ne, LANES), F32)], axis=0)
    cnt_ref[...] = full.T[0:8, :]


def route_call(half, idx, ne, cap):
    nb = idx.shape[0] // LANES
    sd = jax.ShapeDtypeStruct
    return pl.pallas_call(
        functools.partial(route_kernel, ne, cap), out_shape=[sd((nb, LANES), jnp.int32), sd((8, LANES), F32)],
        in_specs=[SM, VM], out_specs=[VM, VM],
        scratch_shapes=[pltpu.VMEM((nb * ne, LANES), F32), pltpu.VMEM((nb * ne, 2 * LANES), F32)], name='route',
        compiler_params=pltpu.CompilerParams(vmem_limit_bytes=VMEM_LIMIT))(half, idx.reshape(nb, LANES))


def dispatch_kernel(nb, tb, ne, cap, d, slot_ref, cnt_ref, x_ref, dy_ref, sx_ref, sdy_ref, tmp, big):
    i = pl.program_id(0)
    nk = d // LANES

    @pl.when(i < nb)
    def _():
        xf = x_ref[...].astype(F32)
        df = dy_ref[...].astype(F32)
        for k in range(nk):
            tmp[pl.ds(k, tb, stride=8), :] = xf[:, k * LANES:(k + 1) * LANES]
            tmp[pl.ds(4 + k, tb, stride=8), :] = df[:, k * LANES:(k + 1) * LANES]

        def place(q, _):
            row = i * (tb // LANES) + q // (LANES // UNROLL)
            col = lax.rem(q, LANES // UNROLL) * UNROLL
            at = [slot_ref[row, col + u] * 8 for u in range(UNROLL)]
            rows = tmp[pl.ds(pl.multiple_of(q * (8 * UNROLL), 8), 8 * UNROLL), :]
            for u in range(UNROLL):
                big[pl.ds(pl.multiple_of(at[u], 8), 8), :] = rows[8 * u:8 * u + 8]
            return 0
        lax.fori_loop(0, tb // UNROLL, place, 0)

    @pl.when(i >= nb)
    def _():
        e = i - nb
        n = cnt_ref[e]
        ok = lax.broadcasted_iota(jnp.int32, (cap, LANES), 0) < n
        base = e * (cap * 8)
        for k in range(nk):
            xk = big[pl.ds(base + k, cap, stride=8), :]
            sx_ref[0, :, k * LANES:(k + 1) * LANES] = jnp.where(ok, xk, 0.0).astype(BF)
            dk = big[pl.ds(base + 4 + k, cap, stride=8), :]
            sdy_ref[0, :, k * LANES:(k + 1) * LANES] = jnp.where(ok, dk, 0.0).astype(BF)


def dispatch_call(slot, cnt, x, dy, ne, cap):
    t, d = x.shape
    tb = 512
    nb = t // tb
    sd = jax.ShapeDtypeStruct((ne, cap, d), BF)
    tok = pl.BlockSpec((tb, d), lambda i: (jnp.minimum(i, nb - 1), 0))
    out = pl.BlockSpec((1, cap, d), lambda i: (jnp.maximum(i - nb, 0), 0, 0))
    return pl.pallas_call(
        functools.partial(dispatch_kernel, nb, tb, ne, cap, d), grid=(nb + ne,), out_shape=[sd, sd],
        in_specs=[SM, SM, tok, tok], out_specs=[out, out],
        scratch_shapes=[pltpu.VMEM((tb * 8, LANES), F32), pltpu.VMEM((ne * cap * 8 + 8, LANES), F32)], name='dispatch',
        compiler_params=pltpu.CompilerParams(vmem_limit_bytes=VMEM_LIMIT))(slot, cnt, x, dy)


def split_router(w_router):
    d, ne = w_router.shape
    hi = lax.reduce_precision(w_router, 8, 7)
    lo = lax.reduce_precision(w_router - hi, 8, 7)
    pad = lambda a: jnp.pad(a, ((0, 0), (0, LANES - ne)))
    wr = jnp.concatenate([pad(hi), pad(lo)], axis=1).astype(BF)
    wrt = jnp.concatenate([pad(hi), pad(hi), pad(lo)], axis=1).T.astype(BF)
    return wr, wrt


def solution(mesh):
    n_dev = mesh.shape['ep']
    hd = n_dev // 2
    mirror = [(i, (i + hd) % n_dev) for i in range(n_dev)]

    def expert_layer(x_tokens, w_router, expert_idx, w_in, w_out, grad_y):
        tokens, d_model = x_tokens.shape
        ff = w_in.shape[-1]
        ne = n_dev
        capacity = (5 * tokens + 4 * ne - 1) // (4 * ne)
        total_tok = tokens * n_dev
        me = lax.axis_index('ep')
        half = me // hd
        w_in_o, w_out_o = w_in[0], w_out[0]
        w_in_m = lax.ppermute(w_in_o, 'ep', mirror)
        wr, wrt = split_router(w_router)

        slot, cnt = route_call(half.reshape(1).astype(jnp.int32), expert_idx, ne, capacity)
        own = cnt[0, :ne].astype(jnp.int32)
        rel_cnt = jnp.where(half == 0, own, jnp.roll(own, hd))
        sx, sdy = dispatch_call(slot, rel_cnt, x_tokens, grad_y, ne, capacity)
        gx, gwi_o, gwo_o, gwi_m, gwo_m, gwr, tot = expert_call(
            (n_dev, hd, capacity, d_model, ff, 512, total_tok), cnt, sx, sdy, w_in_o, w_out_o, w_in_m, wr, wrt)
        grad_x, gwi_r, gwo_r, fin = finish_call(slot, gx, gwi_m, gwo_m, x_tokens, tot, wr, wrt, gwr, total_tok)
        fin = fin[:ne * 8].reshape(ne, 8, LANES)
        nk = d_model // LANES
        grad_w_router = fin[:, :nk].reshape(ne, d_model).T
        aux_loss = AUX_WEIGHT * ne * jnp.sum(tot[0, :ne] / total_tok * fin[0, nk, :ne] / total_tok)
        z_loss = Z_WEIGHT * fin[0, nk + 1, 0] / total_tok
        return grad_x, (gwi_o + gwi_r)[None], (gwo_o + gwo_r)[None], grad_w_router, aux_loss, z_loss

    return jax.shard_map(expert_layer, mesh=mesh,
                         in_specs=(P('ep', None), P(None, None), P('ep'), P('ep', None, None), P('ep', None, None), P('ep', None)),
                         out_specs=(P('ep', None), P('ep', None, None), P('ep', None, None), P(None, None), P(), P()),
                         check_vma=False)
```

```python
import functools
import jax
import jax.numpy as jnp
from jax import lax
from jax.experimental import pallas as pl
from jax.experimental.pallas import tpu as pltpu
from jax.sharding import PartitionSpec as P

AUX_WEIGHT = 0.01
Z_WEIGHT = 0.001
BF = jnp.bfloat16
F32 = jnp.float32
LANES = 128
MESH_ID = pl.DeviceIdType.MESH
VMEM_LIMIT = 60 * 1024 * 1024
UNROLL = 32
SLAB = 4
VM = pl.BlockSpec(memory_space=pltpu.VMEM)
SM = pl.BlockSpec(memory_space=pltpu.SMEM)
HBM = pl.BlockSpec(memory_space=pltpu.HBM)


def xor3(a, b):
    out = 0
    for k in (1, 2, 4):
        out = out + k * lax.rem(a // k + b // k, 2)
    return out


def hop(i):
    odd = lax.rem(i, 2)
    j = (1 - odd) * (7 - i // 2) + odd * ((i + 1) // 2)
    return j - 7 * (1 - (i + 7) // 8) + 3 * (i // 7)


def dot(a, b, ca=1, cb=0):
    return lax.dot_general(a, b, (((ca,), (cb,)), ((), ())), preferred_element_type=F32)


def expert_kernel(cfg, *refs):
    n_dev, hd, cap, d, ff, ft, total_tok = cfg
    (cnt_ref, sx, sdy, wi_o, wo_o, wi_m, wr, wrt,
     gx_out, gwi_o, gwo_o, gwi_m, gwo_m, gwr, tot_ref,
     cbuf, wo_m, xr, dyr, gwot, dlw, oacc, dracc, gb, xt, gt,
     csend, crecv, loc_sem, send_sem, recv_sem, out_sem, w_send, w_recv) = refs
    me = lax.axis_index('ep')
    half = me // hd
    rank = lax.rem(me, hd)
    chip = rank // 2
    core = lax.rem(rank, 2)
    n_grp = hd // 2
    rows = 2 * cap
    twin = rank + 1 - 2 * core
    mirror = lax.rem(me + hd, n_dev)

    def peer_of(j, c):
        return xor3(chip, hop(j)) * 2 + lax.rem(core + c, 2)

    def token_copy(part, a, peer, slot):
        src, dst = ((sx, xr), (sdy, dyr))[a]
        off = part * hd
        return pltpu.make_async_remote_copy(
            src_ref=src.at[off + peer], dst_ref=dst.at[off + slot], send_sem=send_sem.at[a, off + peer],
            recv_sem=recv_sem.at[a, off + slot], device_id=(half * hd + peer,), device_id_type=MESH_ID)

    def count_copy(k, sending):
        peer = lax.rem(me + k, n_dev)
        slot = me if sending else peer
        return pltpu.make_async_remote_copy(
            src_ref=cnt_ref, dst_ref=cbuf.at[slot], send_sem=csend.at[peer],
            recv_sem=crecv.at[slot], device_id=(peer,), device_id_type=MESH_ID)

    def others(fn):
        def body(k, _):
            fn(k)
            return 0
        lax.fori_loop(1, n_dev, body, 0)

    def each(fn):
        fn(twin)

        def body(j, _):
            fn(peer_of(j, 0))
            fn(peer_of(j, 1))
            return 0
        lax.fori_loop(1, n_grp, body, 0)

    weight = pltpu.make_async_remote_copy(src_ref=wo_o, dst_ref=wo_m, send_sem=w_send, recv_sem=w_recv,
                                          device_id=(mirror,), device_id_type=MESH_ID)
    others(lambda k: count_copy(k, True).start())
    cbuf[me] = cnt_ref[...]
    own = [pltpu.make_async_copy(src.at[q * hd + rank], dst.at[q * hd + rank], loc_sem.at[q, a])
           for q in (0, 1) for a, (src, dst) in enumerate(((sx, xr), (sdy, dyr)))]
    for c in own:
        c.start()

    def start(part):
        def one(peer):
            token_copy(part, 0, peer, rank).start()
            token_copy(part, 1, peer, rank).start()
        each(one)
    weight.start()
    start(0)
    start(1)

    gwr[...] = jnp.zeros_like(gwr)
    others(lambda k: count_copy(k, False).wait_recv())
    tot_ref[...] = jnp.sum(cbuf[...], axis=0)
    v = tot_ref[0:1, :] * (AUX_WEIGHT * n_dev / (float(total_tok) * total_tok))
    zc = 2.0 * Z_WEIGHT / total_tok

    for part, (e_id, wi, wo, gwi, gwo) in enumerate(((me, wi_o, wo_o, gwi_o, gwo_o), (mirror, wi_m, wo_m, gwi_m, gwo_m))):
        gwi[...] = jnp.zeros_like(gwi)
        gwot[...] = jnp.zeros_like(gwot)
        if part:
            weight.wait_recv()

        def recv_wait(peer):
            token_copy(part, 0, peer, peer).wait_recv()
            token_copy(part, 1, peer, peer).wait_recv()

        def group(j, _):
            @pl.when(j == 0)
            def _():
                own[2 * part].wait()
                own[2 * part + 1].wait()

            @pl.when(j > 0)
            def _():
                recv_wait(peer_of(j, 0))
            recv_wait(peer_of(j, 1))
            pair = part * n_grp + xor3(chip, hop(j))
            two = pl.ds(2 * pair, 2)
            x = xr[two].reshape(rows, d)
            dyf = dyr[two].reshape(rows, d).astype(F32)
            lane = lax.broadcasted_iota(jnp.int32, (rows, LANES), 1)
            p, lz = router_rows(x, wr, lane, n_dev)
            hot = (lane == e_id).astype(F32)
            gate = jnp.sum(p * hot, axis=1, keepdims=True)
            g = (gate * dyf).astype(BF)
            gb[...] = g
            xt[...] = x.T
            gt[...] = g.T
            oacc[...] = jnp.zeros_like(oacc)
            dracc[...] = jnp.zeros_like(dracc)

            def ff_tile(f, _):
                fo = pl.multiple_of(f * ft, ft)
                wit = wi[:, pl.ds(fo, ft)]
                wot = wo[pl.ds(fo, ft), :]
                xx = xr[two].reshape(rows, d)
                h = jnp.maximum(dot(xx, wit), 0.0).astype(BF)
                oacc[...] += dot(h, wot)
                dh = dot(gb[...], wot, 1, 1)
                da = jnp.where(h > 0, dh, 0.0).astype(BF)
                dracc[...] += dot(da, wit, 1, 1)
                gwot[:, pl.ds(fo, ft)] += dot(gt[...], h)
                gwi[:, pl.ds(fo, ft)] += dot(xt[...], da)
                return 0
            lax.fori_loop(0, ff // ft, ff_tile, 0)

            o = oacc[...].astype(BF).astype(F32)
            dgate = jnp.sum(o * dyr[two].reshape(rows, d).astype(F32), axis=1, keepdims=True)
            dl = (gate * dgate) * (hot - p) + base_grad(p, lz, v, zc)
            dl2, dl3 = split_rows(dl)
            dlw[...] = dot(dl3, wrt[...])
            gw = dot(xt[...], dl2)
            gwr[...] += gw[:, :LANES] + gw[:, LANES:]
            gx = (dracc[...].astype(BF).astype(F32) + dlw[...]).astype(BF)
            dyr[two] = gx.reshape(2, cap, d)
            pltpu.make_async_copy(dyr.at[two], gx_out.at[two], out_sem.at[pair]).start()
            return 0
        lax.fori_loop(0, n_grp, group, 0)

        def finish(f, _):
            fo = pl.multiple_of(f * ft, ft)
            gwo[pl.ds(fo, ft), :] = gwot[:, pl.ds(fo, ft)].T
            return 0
        lax.fori_loop(0, ff // ft, finish, 0)

    for part in (0, 1):
        def drain(peer):
            token_copy(part, 0, peer, peer).wait_send()
            token_copy(part, 1, peer, peer).wait_send()
        each(drain)
    weight.wait_send()

    def out_wait(s, _):
        pltpu.make_async_copy(dyr.at[pl.ds(2 * s, 2)], gx_out.at[pl.ds(2 * s, 2)], out_sem.at[s]).wait()
        return 0
    lax.fori_loop(0, 2 * n_grp, out_wait, 0)
    others(lambda k: count_copy(k, False).wait_send())


def router_rows(x, wr, lane, n_dev):
    lg = dot(x, wr[...])
    lg = jnp.where(lane < n_dev, lg[:, :LANES] + lg[:, LANES:], -1e30)
    mx = jnp.max(lg, axis=1, keepdims=True)
    ex = jnp.exp(lg - mx)
    sm = jnp.sum(ex, axis=1, keepdims=True)
    return ex / sm, mx + jnp.log(sm)


def base_grad(p, lz, v, zc):
    spread = jnp.sum(p * v, axis=1, keepdims=True)
    return p * (v - spread) + (zc * lz) * p


def split_rows(dl):
    hi = dl.astype(BF)
    lo = (dl - hi.astype(F32)).astype(BF)
    dl2 = jnp.concatenate([hi, lo], axis=1)
    return dl2, jnp.concatenate([dl2, hi], axis=1)


def expert_call(cfg, *args):
    n_dev, hd, cap, d, ff, ft, total_tok = cfg
    sd = jax.ShapeDtypeStruct
    rows = 2 * cap
    dma = pltpu.SemaphoreType.DMA
    vf = lambda *shape: pltpu.VMEM(shape, F32)
    vb = lambda *shape: pltpu.VMEM(shape, BF)
    scratch = [vf(n_dev, 8, LANES), vb(ff, d), vb(n_dev, cap, d), vb(n_dev, cap, d), vf(d, ff), vf(rows, d), vf(rows, d), vf(rows, d),
               vb(rows, d), vb(d, rows), vb(d, rows), dma((n_dev,)), dma((n_dev,)), dma((2, 2)), dma((2, n_dev)), dma((2, n_dev)),
               dma((hd,)), dma, dma]
    wi, wo = sd((d, ff), F32), sd((ff, d), F32)
    return pl.pallas_call(
        functools.partial(expert_kernel, cfg),
        out_shape=[sd((n_dev, cap, d), BF), wi, wo, wi, wo, sd((d, LANES), F32), sd((8, LANES), F32)],
        in_specs=[VM, HBM, HBM] + [VM] * 5, out_specs=[HBM] + [VM] * 6, scratch_shapes=scratch, name='experts',
        cost_estimate=pl.CostEstimate(flops=24 * hd * cap * d * ff, bytes_accessed=64 * 2 ** 20, transcendentals=0),
        compiler_params=pltpu.CompilerParams(has_side_effects=True, vmem_limit_bytes=VMEM_LIMIT))(*args)


def finish_kernel(cfg, slot_sm, rows, gwi, gwo, x_ref, slot, tot_ref, wr, wrt, gwr, gx_ref, gwi_r, gwo_r, fin,
                  x_buf, x_sem, bo, bm, big, tmp, acc, part, red, loc_sem, send_sem, recv_sem, rs_send, rs_recv, ag_send, ag_recv,
                  gr_send, gr_recv):
    hd, n_dev, cap, tb, total_tok = cfg
    me = lax.axis_index('ep')
    half = me // hd
    rank = lax.rem(me, hd)
    chip = rank // 2
    core = lax.rem(rank, 2)
    t, d = x_ref.shape
    nk = d // LANES

    def peer_of(j, c):
        return xor3(chip, hop(j)) * 2 + lax.rem(core + c, 2)

    def row_copy(a, peer, slot):
        dst = (bo, bm)[a]
        return pltpu.make_async_remote_copy(
            src_ref=rows.at[a * hd + peer], dst_ref=dst.at[slot], send_sem=send_sem.at[a, peer],
            recv_sem=recv_sem.at[a, slot], device_id=(half * hd + peer,), device_id_type=MESH_ID)

    own = [pltpu.make_async_copy(rows.at[a * hd + rank], b.at[rank], loc_sem.at[a]) for a, b in enumerate((bo, bm))]

    def grad_copy(a):
        src, dst = ((gwo, gwo_r), (gwi, gwi_r))[a]
        return pltpu.make_async_remote_copy(
            src_ref=src, dst_ref=dst, send_sem=gr_send.at[a], recv_sem=gr_recv.at[a],
            device_id=(lax.rem(me + hd, n_dev),), device_id_type=MESH_ID)

    def put(buf, base, s):
        f = buf[s].astype(F32)
        at = pl.ds((base + s) * cap, cap)
        for k in range(nk):
            big[at, k, :] = f[:, k * LANES:(k + 1) * LANES]
        big[at, nk, :] = jnp.zeros((cap, LANES), F32)

    def start(peer):
        for a in (0, 1):
            row_copy(a, peer, rank).start()

    def wait(peer):
        for a in (0, 1):
            row_copy(a, peer, peer).wait_recv()
            put((bo, bm)[a], a * hd, peer)

    def drain(peer):
        for a in (0, 1):
            row_copy(a, peer, peer).wait_send()

    def each(fn):
        fn(rank + 1 - 2 * core)

        def body(j, _):
            fn(peer_of(j, 0))
            fn(peer_of(j, 1))
            return 0
        lax.fori_loop(1, hd // 2, body, 0)
    each(start)
    grad_copy(0).start()
    fetch_x = pltpu.make_async_copy(x_ref, x_buf, x_sem)
    fetch_x.start()
    for c in own:
        c.start()

    v = tot_ref[0:1, :] * (AUX_WEIGHT * n_dev / (float(total_tok) * total_tok))
    acc[...] = gwr[...]
    red[...] = jnp.zeros_like(red)
    fetch_x.wait()

    def block(b, _):
        at = pl.ds(pl.multiple_of(b * tb, tb), tb)
        x = x_buf[at, :]
        lane = lax.broadcasted_iota(jnp.int32, (tb, LANES), 1)
        p, lz = router_rows(x, wr, lane, n_dev)
        dl = base_grad(p, lz, v, 2.0 * Z_WEIGHT / total_tok)
        dl2, dl3 = split_rows(dl)
        gx_ref[at, :] = dot(dl3, wrt[...]).astype(BF)
        drop = (slot[pl.ds(b, 1), :] >= n_dev * cap).astype(F32)
        drop = jnp.broadcast_to(drop, (LANES, LANES)).T.astype(BF)
        gw = dot(x.T, dl2 * jnp.concatenate([drop, drop], axis=1))
        acc[...] += gw[:, :LANES] + gw[:, LANES:]
        red[0:1, :] += jnp.sum(p, axis=0, keepdims=True)
        red[1:2, :] += jnp.sum(jnp.broadcast_to(lz * lz, (tb, LANES)), axis=0, keepdims=True)
        return 0
    lax.fori_loop(0, t // tb, block, 0)

    gt = acc[...].T
    part[...] = jnp.zeros_like(part)
    for k in range(nk):
        part[pl.ds(k, n_dev, stride=8), :] = gt[0:n_dev, k * LANES:(k + 1) * LANES]
    for k in (0, 1):
        part[pl.ds(nk + k, n_dev, stride=8), :] = jnp.broadcast_to(red[k:k + 1, :], (n_dev, LANES))

    def tile(ref, i):
        return ref.at[pl.ds(pl.multiple_of(i * 8, 8), 8)]

    def rs_copy(k, slot):
        peer = lax.rem(me + k, n_dev)
        at = me if slot else peer
        return pltpu.make_async_remote_copy(
            src_ref=tile(part, peer), dst_ref=tile(fin, n_dev + at), send_sem=rs_send.at[peer],
            recv_sem=rs_recv.at[at], device_id=(peer,), device_id_type=MESH_ID)

    def ag_copy(k, slot):
        peer = lax.rem(me + k, n_dev)
        at = me if slot else peer
        return pltpu.make_async_remote_copy(
            src_ref=red, dst_ref=tile(fin, at), send_sem=ag_send.at[peer],
            recv_sem=ag_recv.at[at], device_id=(peer,), device_id_type=MESH_ID)

    def others(fn):
        def body(k, _):
            fn(k)
            return 0
        lax.fori_loop(1, n_dev, body, 0)
    others(lambda k: rs_copy(k, True).start())
    grad_copy(1).start()
    for c in own:
        c.wait()
    put(bo, 0, rank)
    put(bm, hd, rank)
    big[n_dev * cap] = jnp.ones((SLAB, LANES), F32)
    each(wait)

    def combine(b, _):
        def fetch(q, _):
            rows = [big[slot_sm[b, q * UNROLL + u]] for u in range(UNROLL)]
            tmp[pl.ds(pl.multiple_of(q * (SLAB * UNROLL), 8), SLAB * UNROLL), :] = jnp.concatenate(rows, axis=0)
            return 0
        lax.fori_loop(0, LANES // UNROLL, fetch, 0)
        at = pl.ds(pl.multiple_of(b * LANES, LANES), LANES)
        drop = tmp[pl.ds(nk, LANES, stride=SLAB), :] > 0.5
        for k in range(nk):
            lanes = slice(k * LANES, (k + 1) * LANES)
            got = tmp[pl.ds(k, LANES, stride=SLAB), :]
            gx_ref[at, lanes] = jnp.where(drop, gx_ref[at, lanes].astype(F32), got).astype(BF)
        return 0
    lax.fori_loop(0, t // LANES, combine, 0)
    mine = pl.ds(pl.multiple_of(me * 8, 8), 8)
    red[...] = part[mine, :]

    def collect(k):
        rs_copy(k, False).wait_recv()
        src = lax.rem(me + k, n_dev)
        red[...] += fin[pl.ds(pl.multiple_of((n_dev + src) * 8, 8), 8), :]
    others(collect)
    others(lambda k: ag_copy(k, True).start())
    fin[mine, :] = red[...]
    others(lambda k: ag_copy(k, False).wait_recv())
    others(lambda k: rs_copy(k, False).wait_send())
    others(lambda k: ag_copy(k, False).wait_send())
    each(drain)
    for a in (0, 1):
        grad_copy(a).wait()


def finish_call(slot, gx, gwi, gwo, x, tot, wr, wrt, gwr, total_tok):
    n_dev, cap, d = gx.shape
    hd = n_dev // 2
    dma = pltpu.SemaphoreType.DMA
    sd = jax.ShapeDtypeStruct
    rows = pltpu.VMEM((hd, cap, d), BF)
    return pl.pallas_call(
        functools.partial(finish_kernel, (hd, n_dev, cap, LANES, total_tok)),
        out_shape=[sd(x.shape, BF), sd(gwi.shape, F32), sd(gwo.shape, F32), sd((2 * n_dev * 8, LANES), F32)],
        in_specs=[SM] + [HBM] * 4 + [VM] * 5, out_specs=[VM, HBM, HBM, VM],
        scratch_shapes=[pltpu.VMEM(x.shape, BF), dma, rows, rows, pltpu.VMEM((n_dev * cap + 1, SLAB, LANES), F32), pltpu.VMEM((LANES * SLAB, LANES), F32),
                        pltpu.VMEM((d, LANES), F32), pltpu.VMEM((n_dev * 8, LANES), F32), pltpu.VMEM((8, LANES), F32),
                        dma((2,)), dma((2, hd)), dma((2, hd))] + [dma((n_dev,))] * 4 + [dma((2,))] * 2, name='finish',
        cost_estimate=pl.CostEstimate(flops=10 ** 10, bytes_accessed=32 * 2 ** 20, transcendentals=0),
        compiler_params=pltpu.CompilerParams(has_side_effects=True, vmem_limit_bytes=VMEM_LIMIT))(
            slot, gx, gwi, gwo, x, slot, tot, wr, wrt, gwr)


def route_kernel(ne, cap, half_ref, idx_ref, slot_ref, cnt_ref, hot, cum):
    nb = idx_ref.shape[0]
    expert = lax.broadcasted_iota(jnp.int32, (ne, LANES), 0)
    shift = half_ref[0] * (ne // 2)
    for b in range(nb):
        hot[b * ne:(b + 1) * ne, :] = (expert == idx_ref[b:b + 1, :]).astype(F32)
    r = lax.broadcasted_iota(jnp.int32, (LANES, 2 * LANES), 0)
    c = lax.broadcasted_iota(jnp.int32, (LANES, 2 * LANES), 1)
    tri = ((r <= c) | (c >= LANES)).astype(F32).astype(BF)
    cum[...] = dot(hot[...].astype(BF), tri)
    carry = jnp.zeros((ne, LANES), F32)
    for b in range(nb):
        block = cum[b * ne:(b + 1) * ne, :]
        pos = jnp.sum(hot[b * ne:(b + 1) * ne, :] * (block[:, :LANES] + carry), axis=0, keepdims=True) - 1.0
        pos = pos.astype(jnp.int32)
        rel = idx_ref[b:b + 1, :] + shift
        rel = jnp.where(rel >= ne, rel - ne, rel)
        slot_ref[b:b + 1, :] = jnp.where(pos < cap, rel * cap + pos, ne * cap)
        carry = carry + block[:, LANES:]
    full = jnp.concatenate([carry, jnp.zeros((LANES - ne, LANES), F32)], axis=0)
    cnt_ref[...] = full.T[0:8, :]


def route_call(half, idx, ne, cap):
    nb = idx.shape[0] // LANES
    sd = jax.ShapeDtypeStruct
    return pl.pallas_call(
        functools.partial(route_kernel, ne, cap), out_shape=[sd((nb, LANES), jnp.int32), sd((8, LANES), F32)],
        in_specs=[SM, VM], out_specs=[VM, VM],
        scratch_shapes=[pltpu.VMEM((nb * ne, LANES), F32), pltpu.VMEM((nb * ne, 2 * LANES), F32)], name='route',
        compiler_params=pltpu.CompilerParams(vmem_limit_bytes=VMEM_LIMIT))(half, idx.reshape(nb, LANES))


def dispatch_kernel(nb, tb, ne, cap, d, slot_ref, cnt_ref, x_ref, dy_ref, sx_ref, sdy_ref, tmp, big):
    i = pl.program_id(0)
    nk = d // LANES

    @pl.when(i < nb)
    def _():
        xf = x_ref[...].astype(F32)
        df = dy_ref[...].astype(F32)
        for k in range(nk):
            tmp[pl.ds(k, tb, stride=8), :] = xf[:, k * LANES:(k + 1) * LANES]
            tmp[pl.ds(4 + k, tb, stride=8), :] = df[:, k * LANES:(k + 1) * LANES]

        def place(q, _):
            row = i * (tb // LANES) + q // (LANES // UNROLL)
            col = lax.rem(q, LANES // UNROLL) * UNROLL
            at = [slot_ref[row, col + u] * 8 for u in range(UNROLL)]
            rows = tmp[pl.ds(pl.multiple_of(q * (8 * UNROLL), 8), 8 * UNROLL), :]
            for u in range(UNROLL):
                big[pl.ds(pl.multiple_of(at[u], 8), 8), :] = rows[8 * u:8 * u + 8]
            return 0
        lax.fori_loop(0, tb // UNROLL, place, 0)

    @pl.when(i >= nb)
    def _():
        for q in (0, 1):
            e = 2 * (i - nb) + q
            ok = lax.broadcasted_iota(jnp.int32, (cap, LANES), 0) < cnt_ref[e]
            base = e * (cap * 8)
            for k in range(nk):
                xk = big[pl.ds(base + k, cap, stride=8), :]
                sx_ref[q, :, k * LANES:(k + 1) * LANES] = jnp.where(ok, xk, 0.0).astype(BF)
                dk = big[pl.ds(base + 4 + k, cap, stride=8), :]
                sdy_ref[q, :, k * LANES:(k + 1) * LANES] = jnp.where(ok, dk, 0.0).astype(BF)


def dispatch_call(slot, cnt, x, dy, ne, cap):
    t, d = x.shape
    tb = 1024
    nb = t // tb
    sd = jax.ShapeDtypeStruct((ne, cap, d), BF)
    tok = pl.BlockSpec((tb, d), lambda i: (jnp.minimum(i, nb - 1), 0))
    out = pl.BlockSpec((2, cap, d), lambda i: (jnp.maximum(i - nb, 0), 0, 0))
    return pl.pallas_call(
        functools.partial(dispatch_kernel, nb, tb, ne, cap, d), grid=(nb + ne // 2,), out_shape=[sd, sd],
        in_specs=[SM, SM, tok, tok], out_specs=[out, out],
        scratch_shapes=[pltpu.VMEM((tb * 8, LANES), F32), pltpu.VMEM((ne * cap * 8 + 8, LANES), F32)], name='dispatch',
        compiler_params=pltpu.CompilerParams(vmem_limit_bytes=VMEM_LIMIT))(slot, cnt, x, dy)


def split_router(w_router):
    d, ne = w_router.shape
    hi = lax.reduce_precision(w_router, 8, 7)
    lo = lax.reduce_precision(w_router - hi, 8, 7)
    pad = lambda a: jnp.pad(a, ((0, 0), (0, LANES - ne)))
    wr = jnp.concatenate([pad(hi), pad(lo)], axis=1).astype(BF)
    wrt = jnp.concatenate([pad(hi), pad(hi), pad(lo)], axis=1).T.astype(BF)
    return wr, wrt


def solution(mesh):
    n_dev = mesh.shape['ep']
    hd = n_dev // 2
    mirror = [(i, (i + hd) % n_dev) for i in range(n_dev)]

    def expert_layer(x_tokens, w_router, expert_idx, w_in, w_out, grad_y):
        tokens, d_model = x_tokens.shape
        ff = w_in.shape[-1]
        ne = n_dev
        capacity = (5 * tokens + 4 * ne - 1) // (4 * ne)
        total_tok = tokens * n_dev
        me = lax.axis_index('ep')
        half = me // hd
        w_in_o, w_out_o = w_in[0], w_out[0]
        w_in_m = lax.ppermute(w_in_o, 'ep', mirror)
        wr, wrt = split_router(w_router)

        slot, cnt = route_call(half.reshape(1).astype(jnp.int32), expert_idx, ne, capacity)
        own = cnt[0, :ne].astype(jnp.int32)
        rel_cnt = jnp.where(half == 0, own, jnp.roll(own, hd))
        sx, sdy = dispatch_call(slot, rel_cnt, x_tokens, grad_y, ne, capacity)
        gx, gwi_o, gwo_o, gwi_m, gwo_m, gwr, tot = expert_call(
            (n_dev, hd, capacity, d_model, ff, 512, total_tok), cnt, sx, sdy, w_in_o, w_out_o, w_in_m, wr, wrt)
        grad_x, gwi_r, gwo_r, fin = finish_call(slot, gx, gwi_m, gwo_m, x_tokens, tot, wr, wrt, gwr, total_tok)
        fin = fin[:ne * 8].reshape(ne, 8, LANES)
        nk = d_model // LANES
        grad_w_router = fin[:, :nk].reshape(ne, d_model).T
        aux_loss = AUX_WEIGHT * ne * jnp.sum(tot[0, :ne] / total_tok * fin[0, nk, :ne] / total_tok)
        z_loss = Z_WEIGHT * fin[0, nk + 1, 0] / total_tok
        return grad_x, (gwi_o + gwi_r)[None], (gwo_o + gwo_r)[None], grad_w_router, aux_loss, z_loss

    return jax.shard_map(expert_layer, mesh=mesh,
                         in_specs=(P('ep', None), P(None, None), P('ep'), P('ep', None, None), P('ep', None, None), P('ep', None)),
                         out_specs=(P('ep', None), P('ep', None, None), P('ep', None, None), P(None, None), P(), P()),
                         check_vma=False)
```
